128 devices in a mesh: blk: 16 (over y_hi, x, core), grp: 8 (over y_lo, z).
Axes of the slice: x: 4, y: 4 (y_hi: 2, y_lo: 2; y = y_hi * 2 + y_lo), z: 4, core: 2. Of those that a mesh axis runs over, the one named last changes fastest.
Arguments:
- trial_vec: float32 [6144, 24], P(('blk', 'grp')), may hold values from -6 to 6
- resid_vec: float32 [6144, 24], P(('blk', 'grp')), may hold values from -6 to 6
- search_dir: float32 [6144, 24], P(('blk', 'grp')), may hold values from -6 to 6
- trial_img: float32 [6144, 24], P(('blk', 'grp')), may hold values from -12 to 12
- search_img: float32 [6144, 24], P(('blk', 'grp')), may hold values from -12 to 12
- dens_exch: bfloat16 [6144, 20480], P(('blk', 'grp')), may hold values from -0.078125 to 0.078125
- dens_direct: bfloat16 [6144, 20480], P(('blk', 'grp')), may hold values from -0.078125 to 0.078125
- screen_mat: bfloat16 [20480, 20480], P('grp', 'blk'), may hold values from -0.0390625 to 0.0390625
- coulomb: float32 [20480], replicated, may hold values from 0.2 to 2
- valence_energy: float32 [96], replicated, may hold values from -3 to -1
- conduct_energy: float32 [256], replicated, may hold values from 0.5 to 3
- valence_index: int32 [6144], P(('blk', 'grp')), may hold values from 0 to 95, as said below
- conduct_index: int32 [6144], P(('blk', 'grp')), may hold values from 0 to 255, as said below
- ritz_coef: float32 [72, 24], replicated, may hold values from -1.75 to 1.75
Outputs:
- next_trial: float32 [6144, 24], P(('blk', 'grp'))
- next_trial_img: float32 [6144, 24], P(('blk', 'grp'))
- next_search: float32 [6144, 24], P(('blk', 'grp'))
- next_search_img: float32 [6144, 24], P(('blk', 'grp'))
- gram_matrix: float32 [72, 72], replicated
The draws below stay inside these ranges and needn't reach their ends.
Inputs may be any that keep to these rules, and one draw needn't show every extreme that they name: `valence_index`: no two pairs have both the same valence band and the same conduction band. `conduct_index`: no two pairs have both the same valence band and the same conduction band.
All inputs are finite; a program needn't handle non-finite values.
Results may differ from the reference program's by a relative error of at most 0.0034.
Values may be sent and summed in bfloat16 or wider, within the bound.
A program may use at most 64 MiB of HBM per device.

```python
import math
import jax
import jax.numpy as jnp
from jax import lax

NG = 20480
NE = 24
NV = 96
NC = 256
PAIRS = 6144


def pair_numbers(key):
    mixed = jax.random.permutation(jax.random.fold_in(key, 7), NV * NC)
    return mixed[:PAIRS].astype(jnp.int32)


def draw_valence_index(key, part):
    return (pair_numbers(key) // NC).astype(jnp.int32)


def draw_conduct_index(key, part):
    return (pair_numbers(key) % NC).astype(jnp.int32)


def level_of(own_key, extent, cuts, low, top_value):
    gain = 1.0
    for position, blocks in cuts:
        draws = jax.random.uniform(jax.random.fold_in(jax.random.fold_in(own_key, 6), position), (blocks,), jnp.float32, low / len(cuts), top_value / len(cuts))
        gain = gain * jnp.repeat(jnp.exp(draws), extent[position] // blocks).reshape((-1,) + (1,) * (len(extent) - 1 - position))
    return gain


def bell_draw(key, dims, width, bound, cuts=(), kind=jnp.bfloat16):
    entries = width * jax.random.normal(key, dims, jnp.float32)
    if cuts:
        entries = entries * level_of(key, dims, cuts, -0.22, 0.18)
    return jnp.clip(entries, -bound, bound).astype(kind)


def setup_inputs(seed: int = 0) -> dict:
    keys = jax.random.split(jax.random.key(seed), 15)
    return {
        "trial_vec": bell_draw(keys[0], (PAIRS, NE), 1.0, 6.0, ((0, 128),), jnp.float32),
        "resid_vec": bell_draw(keys[1], (PAIRS, NE), 1.0, 6.0, ((0, 128),), jnp.float32),
        "search_dir": bell_draw(keys[2], (PAIRS, NE), 1.0, 6.0, ((0, 128),), jnp.float32),
        "trial_img": bell_draw(keys[3], (PAIRS, NE), 2.0, 12.0, ((0, 128),), jnp.float32),
        "search_img": bell_draw(keys[4], (PAIRS, NE), 2.0, 12.0, ((0, 128),), jnp.float32),
        "dens_exch": bell_draw(keys[5], (PAIRS, NG), PAIRS ** -0.5, 0.078125, ((0, 128),)),
        "dens_direct": bell_draw(keys[6], (PAIRS, NG), PAIRS ** -0.5, 0.078125, ((0, 128),)),
        "screen_mat": bell_draw(keys[7], (NG, NG), NG ** -0.5, 0.0390625, ((0, 8), (1, 16))),
        "coulomb": jnp.clip(jnp.exp(jax.random.uniform(keys[8], (NG,), jnp.float32, math.log(0.2), math.log(2.0))), 0.2, 2.0),
        "valence_energy": jnp.clip(jax.random.uniform(keys[9], (NV,), jnp.float32, -3.0, -1.0), -3.0, -1.0),
        "conduct_energy": jnp.clip(jax.random.uniform(keys[10], (NC,), jnp.float32, 0.5, 3.0), 0.5, 3.0),
        "valence_index": draw_valence_index(jax.random.fold_in(keys[14], 71), 0),
        "conduct_index": draw_conduct_index(jax.random.fold_in(keys[14], 71), 0),
        "ritz_coef": bell_draw(keys[13], (3 * NE, NE), 0.3, 1.75, (), jnp.float32),
    }


def tdot(left, right):
    return jnp.dot(left, right, precision=lax.Precision.HIGHEST)


def reference(trial_vec, resid_vec, search_dir, trial_img, search_img, dens_exch, dens_direct, screen_mat, coulomb, valence_energy, conduct_energy, valence_index, conduct_index, ritz_coef):
    gap = conduct_energy[conduct_index.astype(jnp.int32)] - valence_energy[valence_index.astype(jnp.int32)]
    resid_half = resid_vec.astype(jnp.bfloat16)
    proj = jnp.dot(dens_exch.T, resid_half, preferred_element_type=jnp.float32)
    weighted = (coulomb[:, None] * proj).astype(jnp.bfloat16)
    exch_term = jnp.dot(dens_exch, weighted, preferred_element_type=jnp.float32)
    seen = jnp.dot(dens_direct.T, resid_half, preferred_element_type=jnp.float32).astype(jnp.bfloat16)
    screened = jnp.dot(screen_mat, seen, preferred_element_type=jnp.float32).astype(jnp.bfloat16)
    direct_term = jnp.dot(dens_direct, screened, preferred_element_type=jnp.float32)
    resid_img = gap[:, None] * resid_vec + 2.0 * exch_term - direct_term
    basis = jnp.concatenate([trial_vec, resid_vec, search_dir], axis=1)
    images = jnp.concatenate([trial_img, resid_img, search_img], axis=1)
    gram_matrix = tdot(basis.T, images)
    lower = ritz_coef[NE:]
    next_trial = tdot(basis, ritz_coef)
    next_trial_img = tdot(images, ritz_coef)
    next_search = tdot(jnp.concatenate([resid_vec, search_dir], axis=1), lower)
    next_search_img = tdot(jnp.concatenate([resid_img, search_img], axis=1), lower)
    return next_trial, next_trial_img, next_search, next_search_img, gram_matrix
```

```python
import jax
import jax.numpy as jnp
from jax import lax
from jax.experimental import pallas as pl
from jax.experimental.pallas import tpu as pltpu
from jax.sharding import PartitionSpec as P

NE = 24
ROWS = 48
NG = 20480
COLS = 640
MESH = pl.DeviceIdType.MESH
FAR = (2, 1, 3)
F32 = jnp.float32
BF16 = jnp.bfloat16
X, R, S = (pl.ds(i * NE, NE) for i in range(3))


NT = ((1,), (1,))


def exact(a, b, dims=((1,), (0,))):
    return lax.dot_general(
        a, b, (dims, ((), ())), precision=lax.Precision.HIGHEST, preferred_element_type=F32
    )


def nt(a, b):
    return lax.dot_general(a, b, (((1,), (1,)), ((), ())), preferred_element_type=F32)


def nn(a, b):
    return lax.dot_general(a, b, (((1,), (0,)), ((), ())), preferred_element_type=F32)


def kernel(
    trial_h, resid_h, search_h, trial_img_h, search_img_h, dens_e_h, dens_d_h, screen_h,
    coulomb_h, val_e_h, con_e_h, val_i_h, con_i_h, ritz_h,
    o_trial, o_trial_img, o_search, o_search_img, o_gram,
    basis, images, dens_e, dens_d, screen, coulomb, val_e, con_e, val_i, con_i, ritz,
    rt, s0s, s0r, acc, s1s, s1r, s2s, s2r, s3s, s3r,
    seen, bacc, c0s, c0r, c1s, c1r, c2s, c2r, gat, early, late,
    ld, s0x, s0y, s1x, s1y, s2x, s2y, s3x, s3y, s4x, s4y,
    c0x, c0y, c1x, c1y, c2x, c2y, a1x, a1y, a2x, a2y, a3x, a3y, ex, ey, lx, ly,
):
    blk = lax.axis_index("blk")
    grp = lax.axis_index("grp")
    c = blk % 2
    x = (blk // 2) % 4
    y_hi = blk // 8
    y_lo = grp // 4
    z = grp % 4
    y = y_hi * 2 + y_lo
    at = {"x": x, "y": y, "z": z}

    def device(x=x, y=y, z=z, c=c):
        return ((y // 2) * 8 + x * 2 + c, (y % 2) * 4 + z)

    def along(axis, step):
        return device(**{axis: (at[axis] + step) % 4})

    other = device(c=1 - c)

    loads = []
    for i, (src, dst) in enumerate((
        (resid_h, basis.at[R]), (dens_d_h, dens_d), (dens_e_h, dens_e), (screen_h, screen),
        (trial_h, basis.at[X]), (search_h, basis.at[S]), (trial_img_h, images.at[X]),
        (search_img_h, images.at[S]), (coulomb_h, coulomb), (val_e_h, val_e), (con_e_h, con_e),
        (val_i_h, val_i), (con_i_h, con_i), (ritz_h, ritz),
    )):
        copy = pltpu.make_async_copy(src, dst, ld.at[i])
        copy.start()
        loads.append(copy)

    barrier = pltpu.get_barrier_semaphore()
    peers = [other] + [along(a, d) for a in "xyz" for d in FAR]
    for peer in peers:
        pl.semaphore_signal(barrier, inc=1, device_id=peer, device_id_type=MESH)

    sends = []

    def send(src, dst, ssem, rsem, dev):
        copy = pltpu.make_async_remote_copy(
            src_ref=src, dst_ref=dst, send_sem=ssem, recv_sem=rsem,
            device_id=dev, device_id_type=MESH,
        )
        copy.start()
        sends.append(copy)

    def landed(ref, rsem, ssem):
        pltpu.make_async_remote_copy(
            src_ref=ref, dst_ref=ref, send_sem=ssem, recv_sem=rsem,
            device_id=other, device_id_type=MESH,
        ).wait_recv()

    STEPS = FAR + (0,)
    dens = (dens_d, dens_e)
    first = ("x", "z")
    third = ("z", "x")

    def lanes(block):
        return pl.ds(pl.multiple_of(block * COLS, COLS), COLS)

    def part_block(p, step1, step2, core):
        a1 = (at[first[p]] + step1) % 4
        a2 = (y + step2) % 4
        return (a2 // 2) * 16 + a1 * 4 + core * 2 + a2 % 2

    loads[0].wait()
    rt[...] = basis[R, :].astype(BF16)

    def core_parts(p):
        loads[1 + p].wait()
        for k in range(4):
            for j in range(4):
                block = part_block(p, STEPS[k], STEPS[j], 1 - c)
                s0s[p, k, j] = nn(rt[...], dens[p][:, lanes(block)]).astype(BF16)
            if p == 0 and k == 0:
                pl.semaphore_wait(barrier, len(peers))
            send(s0s.at[p, k], s0r.at[p, k], s0x.at[p, k], s0y.at[p, k], other)

    def own_parts(p):
        for k in range(4):
            for j in range(4):
                block = part_block(p, STEPS[k], STEPS[j], c)
                acc[p, k, j] = nn(rt[...], dens[p][:, lanes(block)])

    def first_axis(p):
        for k in range(4):
            landed(s0r.at[p, k], s0y.at[p, k], s0x.at[p, k])
            for j in range(4):
                v = acc[p, k, j] + s0r[p, k, j].astype(F32)
                if k == 3:
                    acc[p, k, j] = v
                else:
                    s1s[p, k, j] = v.astype(BF16)
                    send(s1s.at[p, k, j], s1r.at[p, k, j], s1x.at[p, k, j], s1y.at[p, k, j],
                         along(first[p], STEPS[k]))

    def second_axis(p):
        for j in range(4):
            v = acc[p, 3, j]
            for k in range(3):
                landed(s1r.at[p, k, j], s1y.at[p, k, j], s1x.at[p, k, j])
                v = v + s1r[p, k, j].astype(F32)
            if j == 3:
                acc[p, 3, j] = v
            else:
                s2s[p, j] = v.astype(BF16)
                send(s2s.at[p, j], s2r.at[p, j], s2x.at[p, j], s2y.at[p, j], along("y", STEPS[j]))

    def third_axis(p):
        v = acc[p, 3, 3]
        for j in range(3):
            landed(s2r.at[p, j], s2y.at[p, j], s2x.at[p, j])
            v = v + s2r[p, j].astype(F32)
        acc[p, 3, 3] = v
        s3s[p] = v.astype(BF16)
        for k in range(3):
            send(s3s.at[p], s3r.at[p, k], s3x.at[p, k], s3y.at[p, k], along(third[p], FAR[k]))

    def total(p):
        v = acc[p, 3, 3]
        for k in range(3):
            landed(s3r.at[p, k], s3y.at[p, k], s3x.at[p, k])
            v = v + s3r[p, k].astype(F32)
        return v

    BACK = (0,) + FAR

    def gat_block(p, stepy, stepz, core):
        yy = (y + 4 - stepy) % 4
        zz = (z + 4 - stepz) % 4
        if p == 0:
            return ((yy % 2) * 4 + zz) * 4 + core * 2 + yy // 2
        return (yy // 2) * 16 + zz * 4 + core * 2 + yy % 2

    def pass_on(p, m, kz, block):
        ref = gat.at[p, block]
        if m == 0 and kz == 0:
            for k in range(3):
                send(ref, ref, a1x.at[p, k], a1y.at[p, k], along("y", FAR[k]))
        if kz == 0:
            for k in range(3):
                send(ref, ref, a2x.at[p, k, m], a2y.at[p, k, m], along("z", FAR[k]))
        send(ref, ref, a3x.at[p, kz, m], a3y.at[p, kz, m], other)

    def use(p, block):
        return nt(gat[p, block], dens[p][:, lanes(block)])

    def gather_mine(p, term):
        block = gat_block(p, 0, 0, c)
        pass_on(p, 0, 0, block)
        part = use(p, block)
        return part if term is None else term + part

    def gather_y(p, term):
        for m in range(1, 4):
            block = gat_block(p, BACK[m], 0, c)
            landed(gat.at[p, block], a1y.at[p, m - 1], a1x.at[p, m - 1])
            pass_on(p, m, 0, block)
            term = term + use(p, block)
        return term

    def gather_z(p, term):
        for m in range(4):
            for kz in range(1, 4):
                block = gat_block(p, BACK[m], BACK[kz], c)
                landed(gat.at[p, block], a2y.at[p, kz - 1, m], a2x.at[p, kz - 1, m])
                pass_on(p, m, kz, block)
                term = term + use(p, block)
        return term

    def gather_core(p, term):
        for m in range(4):
            for kz in range(4):
                block = gat_block(p, BACK[m], BACK[kz], 1 - c)
                landed(gat.at[p, block], a3y.at[p, kz, m], a3x.at[p, kz, m])
                term = term + use(p, block)
        return term

    def share(buf, ssem, rsem, s, value):
        axis = "cxyz"[s]
        count = 2 if axis == "c" else 4
        here = c if axis == "c" else at[axis]
        buf[s, here] = value
        for k in range(count - 1):
            dev = other if axis == "c" else along(axis, FAR[k])
            send(buf.at[s, here], buf.at[s, here], ssem.at[s, k], rsem.at[s, here], dev)

    def shared(buf, ssem, rsem, s):
        axis = "cxyz"[s]
        count = 2 if axis == "c" else 4
        here = c if axis == "c" else at[axis]
        for k in range(count - 1):
            there = 1 - c if axis == "c" else (here + FAR[k]) % 4
            landed(buf.at[s, there], rsem.at[s, there], ssem.at[s, k])
        value = buf[s, 0]
        for i in range(1, count):
            value = value + buf[s, i]
        return value

    with jax.named_scope("core_d"):
        core_parts(0)
    with jax.named_scope("own_d"):
        own_parts(0)
    with jax.named_scope("first_d"):
        first_axis(0)
    with jax.named_scope("core_e"):
        core_parts(1)
    with jax.named_scope("own_e"):
        own_parts(1)
    with jax.named_scope("first_e"):
        first_axis(1)
    with jax.named_scope("early"):
        for i in (4, 5, 6, 7, 9, 10, 11, 12, 13):
            loads[i].wait()
        share(early, ex, ey, 0, jnp.concatenate(
            [exact(images[X, :], basis[...], NT), exact(images[S, :], basis[...], NT)], axis=0))
    with jax.named_scope("second_d"):
        second_axis(0)
    with jax.named_scope("second_e"):
        second_axis(1)
    with jax.named_scope("third_d"):
        third_axis(0)
    with jax.named_scope("third_e"):
        third_axis(1)
    share(early, ex, ey, 1, shared(early, ex, ey, 0))

    with jax.named_scope("seen"):
        tot = total(0)
        seen[y_lo] = tot.astype(BF16)
        send(seen.at[y_lo], seen.at[y_lo], s4x, s4y, along("y", 5 - 2 * y_lo))
    with jax.named_scope("mm_near"):
        loads[3].wait()
        for q in range(4):
            bacc[q] = nt(seen[y_lo], screen[pl.ds(q * COLS, COLS), lanes(y_lo)])

    with jax.named_scope("weighted"):
        tot = total(1)
        loads[8].wait()
        mine = gat_block(1, 0, 0, c)
        gat[1, mine] = (coulomb[:, lanes(mine)] * tot).astype(BF16)
        exch = gather_mine(1, None)

    def rest(q):
        rows = pl.ds(pl.multiple_of(q * COLS, COLS), COLS)
        return bacc[q] + nt(seen[1 - y_lo], screen[rows, lanes(1 - y_lo)])

    with jax.named_scope("mm_far"):
        landed(seen.at[1 - y_lo], s4y, s4x)
        for i in range(2):
            c0s[i] = rest((1 - c) * 2 + i).astype(BF16)
            send(c0s.at[i], c0r.at[i], c0x.at[i], c0y.at[i], other)
        away = rest(c * 2 + 1 - y_hi)
        home = rest(c * 2 + y_hi)

    with jax.named_scope("c0"):
        for i in range(2):
            landed(c0r.at[i], c0y.at[i], c0x.at[i])
        c1s[...] = (away + c0r[1 - y_hi].astype(F32)).astype(BF16)
        send(c1s, c1r, c1x, c1y, along("y", 2))
        home = home + c0r[y_hi].astype(F32)

    share(early, ex, ey, 2, shared(early, ex, ey, 1))
    with jax.named_scope("gather_y_e"):
        exch = gather_y(1, exch)

    with jax.named_scope("c1"):
        landed(c1r, c1y, c1x)
        home = home + c1r[...].astype(F32)
        c2s[...] = home.astype(BF16)
        for k in range(3):
            send(c2s, c2r.at[k], c2x.at[k], c2y.at[k], along("x", FAR[k]))

    share(early, ex, ey, 3, shared(early, ex, ey, 2))
    with jax.named_scope("gather_z_e"):
        exch = gather_z(1, exch)

    with jax.named_scope("c2"):
        for k in range(3):
            landed(c2r.at[k], c2y.at[k], c2x.at[k])
            home = home + c2r[k].astype(F32)
        mine = gat_block(0, 0, 0, c)
        gat[0, mine] = home.astype(BF16)
        direct = gather_mine(0, None)

    with jax.named_scope("gather_core_e"):
        exch = gather_core(1, exch)

    with jax.named_scope("plain"):
        def pick(energy, index, count):
            hot = (lax.broadcasted_iota(jnp.int32, (count, ROWS), 0) == index[...]).astype(F32)
            return exact(energy[...], hot)

        gap = pick(con_e, con_i, con_e.shape[1]) - pick(val_e, val_i, val_e.shape[1])
        near = gap * basis[R, :] + 2.0 * exch
        all_coef = ritz[...]
        column = lax.broadcasted_iota(jnp.int32, all_coef.shape, 1)
        lower = jnp.where(column >= NE, all_coef, 0.0)
        o_trial[...] = exact(all_coef, basis[...])
        o_search[...] = exact(lower, basis[...])

    with jax.named_scope("gather_y_d"):
        direct = gather_y(0, direct)
    gram = shared(early, ex, ey, 3)
    with jax.named_scope("gather_z_d"):
        direct = gather_z(0, direct)
    with jax.named_scope("gather_core_d"):
        direct = gather_core(0, direct)

    with jax.named_scope("image"):
        resid_img = near - direct
        share(late, lx, ly, 0, exact(resid_img, basis[...], NT))
        images[R, :] = resid_img
        o_trial_img[...] = exact(all_coef, images[...])
        o_search_img[...] = exact(lower, images[...])
    for s in range(1, 4):
        with jax.named_scope(f"late{s}"):
            share(late, lx, ly, s, shared(late, lx, ly, s - 1))
    with jax.named_scope("late4"):
        mid = shared(late, lx, ly, 3)
        gram = jnp.concatenate([gram[0:NE], mid, gram[NE:2 * NE]], axis=0)
        o_gram[...] = jnp.transpose(gram)

    with jax.named_scope("drain"):
        for copy in sends:
            copy.wait_send()


def put(*refs):
    n = len(refs) // 2
    sem = refs[-1]
    copies = [pltpu.make_async_copy(refs[i], refs[n + i], sem.at[i]) for i in range(n)]
    for copy in copies:
        copy.start()
    for copy in copies:
        copy.wait()


def solution(mesh):
    def body(trial, resid, search, trial_img, search_img, dens_e, dens_d, screen,
             coulomb, val_e, con_e, val_i, con_i, ritz):
        args = (trial.T, resid.T, search.T, trial_img.T, search_img.T, dens_e, dens_d, screen,
                coulomb.reshape(1, -1), val_e.reshape(1, -1), con_e.reshape(1, -1),
                val_i.reshape(1, -1), con_i.reshape(1, -1), ritz.T)
        dma = pltpu.SemaphoreType.DMA
        block = (NE, COLS)
        tall = pltpu.VMEM((3 * NE, ROWS), F32)
        scratch = [tall, tall] + [pltpu.VMEM(a.shape, a.dtype) for a in args[5:]] + [
            pltpu.VMEM((NE, ROWS), BF16),
            pltpu.VMEM((2, 4, 4) + block, BF16),
            pltpu.VMEM((2, 4, 4) + block, BF16),
            pltpu.VMEM((2, 4, 4) + block, F32),
            pltpu.VMEM((2, 3, 4) + block, BF16),
            pltpu.VMEM((2, 3, 4) + block, BF16),
            pltpu.VMEM((2, 3) + block, BF16),
            pltpu.VMEM((2, 3) + block, BF16),
            pltpu.VMEM((2,) + block, BF16),
            pltpu.VMEM((2, 3) + block, BF16),
            pltpu.VMEM((2,) + block, BF16),
            pltpu.VMEM((4,) + block, F32),
            pltpu.VMEM((2,) + block, BF16),
            pltpu.VMEM((2,) + block, BF16),
            pltpu.VMEM(block, BF16),
            pltpu.VMEM(block, BF16),
            pltpu.VMEM(block, BF16),
            pltpu.VMEM((3,) + block, BF16),
            pltpu.VMEM((2, 32) + block, BF16),
            pltpu.VMEM((4, 4, 2 * NE, 3 * NE), F32),
            pltpu.VMEM((4, 4, NE, 3 * NE), F32),
            dma((14,)),
            dma((2, 4)), dma((2, 4)),
            dma((2, 3, 4)), dma((2, 3, 4)),
            dma((2, 3)), dma((2, 3)),
            dma((2, 3)), dma((2, 3)),
            dma, dma,
            dma((2,)), dma((2,)),
            dma, dma,
            dma((3,)), dma((3,)),
            dma((2, 3)), dma((2, 3)),
            dma((2, 3, 4)), dma((2, 3, 4)),
            dma((2, 4, 4)), dma((2, 4, 4)),
            dma((4, 3)), dma((4, 4)),
            dma((4, 3)), dma((4, 4)),
        ]
        vec = jax.ShapeDtypeStruct((NE, ROWS), F32)
        outs = (vec, vec, vec, vec, jax.ShapeDtypeStruct((3 * NE, 3 * NE), F32))
        parts = pl.pallas_call(
            kernel,
            out_shape=outs,
            in_specs=[pl.BlockSpec(memory_space=pl.ANY)] * len(args),
            out_specs=[pl.BlockSpec(memory_space=pltpu.VMEM)] * 5,
            scratch_shapes=scratch,
            compiler_params=pltpu.CompilerParams(
                collective_id=0, has_side_effects=True, vmem_limit_bytes=67043328
            ),
            name="step",
        )(*args)
        parts = pl.pallas_call(
            put,
            out_shape=outs,
            in_specs=[pl.BlockSpec(memory_space=pltpu.VMEM)] * 5,
            out_specs=[pl.BlockSpec(memory_space=pl.ANY)] * 5,
            scratch_shapes=[dma((5,))],
            name="put",
        )(*parts)
        return tuple(a.T for a in parts[:4]) + (parts[4],)

    both = P(("blk", "grp"), None)
    one = P(("blk", "grp"))
    return jax.shard_map(
        body,
        mesh=mesh,
        in_specs=(both,) * 7 + (P("grp", "blk"), P(None), P(None), P(None), one, one, P(None, None)),
        out_specs=(both,) * 4 + (P(None, None),),
        check_vma=False,
    )
```

```python
import jax
import jax.numpy as jnp
from jax import lax
from jax.experimental import pallas as pl
from jax.experimental.pallas import tpu as pltpu
from jax.sharding import PartitionSpec as P

NE = 24
ROWS = 48
NG = 20480
COLS = 640
MESH = pl.DeviceIdType.MESH
FAR = (2, 1, 3)
F32 = jnp.float32
BF16 = jnp.bfloat16
X, R, S = (pl.ds(i * NE, NE) for i in range(3))


NT = ((1,), (1,))


def exact(a, b, dims=((1,), (0,))):
    return lax.dot_general(
        a, b, (dims, ((), ())), precision=lax.Precision.HIGHEST, preferred_element_type=F32
    )


def nt(a, b):
    return lax.dot_general(a, b, (((1,), (1,)), ((), ())), preferred_element_type=F32)


def nn(a, b):
    return lax.dot_general(a, b, (((1,), (0,)), ((), ())), preferred_element_type=F32)


def kernel(
    trial_h, resid_h, search_h, trial_img_h, search_img_h, dens_e_h, dens_d_h, screen_h,
    coulomb_h, val_e_h, con_e_h, val_i_h, con_i_h, ritz_h,
    h_trial, h_trial_img, h_search, h_search_img, h_gram,
    o_trial, o_trial_img, o_search, o_search_img, o_gram,
    basis, images, dens_e, dens_d, screen, coulomb, val_e, con_e, val_i, con_i, ritz,
    rt, s0s, s0r, acc, rls, rlr, s1s, s1r, s2s, s2r, s3s, s3r,
    qb, seen, bacc, c0s, c0r, c1s, c1r, c2s, c2r, gat, early, late,
    ld, st, sx, ex, lx, s0y, s0q, rly, rlq, s1y, s1q, s2y, s3y, s4y, c0y, c1y, c2y,
    a1y, a2y, a3y, ey, ly,
):
    blk = lax.axis_index("blk")
    grp = lax.axis_index("grp")
    c = blk % 2
    x = (blk // 2) % 4
    y_hi = blk // 8
    y_lo = grp // 4
    z = grp % 4
    y = y_hi * 2 + y_lo
    at = {"x": x, "y": y, "z": z}

    def device(x=x, y=y, z=z, c=c):
        return ((y // 2) * 8 + x * 2 + c, (y % 2) * 4 + z)

    def along(axis, step):
        return device(**{axis: (at[axis] + step) % 4})

    other = device(c=1 - c)

    loads = []
    for i, (src, dst) in enumerate((
        (resid_h, basis.at[R]), (dens_d_h, dens_d), (dens_e_h, dens_e), (screen_h, screen),
        (trial_h, basis.at[X]), (search_h, basis.at[S]), (trial_img_h, images.at[X]),
        (search_img_h, images.at[S]), (coulomb_h, coulomb), (val_e_h, val_e), (con_e_h, con_e),
        (val_i_h, val_i), (con_i_h, con_i), (ritz_h, ritz),
    )):
        copy = pltpu.make_async_copy(src, dst, ld.at[i])
        copy.start()
        loads.append(copy)

    barrier = pltpu.get_barrier_semaphore()
    peers = [other] + [along(a, d) for a in "xyz" for d in FAR]
    for peer in peers:
        pl.semaphore_signal(barrier, inc=1, device_id=peer, device_id_type=MESH)

    stores = []

    def store(i, src, dst):
        copy = pltpu.make_async_copy(src, dst, st.at[i])
        copy.start()
        stores.append(copy)

    def send(src, dst, ssem, rsem, dev):
        copy = pltpu.make_async_remote_copy(
            src_ref=src, dst_ref=dst, send_sem=ssem, recv_sem=rsem,
            device_id=dev, device_id_type=MESH,
        )
        copy.start()

    def landed(ref, rsem):
        pltpu.make_async_remote_copy(
            src_ref=ref, dst_ref=ref, send_sem=sx.at[0], recv_sem=rsem,
            device_id=other, device_id_type=MESH,
        ).wait_recv()

    def left(ref, ssem):
        pltpu.make_async_remote_copy(
            src_ref=ref, dst_ref=ref, send_sem=ssem, recv_sem=s4y,
            device_id=other, device_id_type=MESH,
        ).wait_send()

    STEPS = FAR + (0,)
    dens = (dens_d, dens_e, dens_d, dens_d, dens_d)
    group = (R, R, X, R, S)
    first = ("x", "z", "z", "z", "z")
    second = ("y",) * 5
    third = ("z", "x")

    def lanes(block):
        return pl.ds(pl.multiple_of(block * COLS, COLS), COLS)

    def part_block(p, step1, step2, core):
        a1 = (at[first[p]] + step1) % 4
        a2 = (at[second[p]] + step2) % 4
        if p == 0:
            return (a2 // 2) * 16 + a1 * 4 + core * 2 + a2 % 2
        if p == 1:
            return core * 16 + a2 * 4 + a1
        return ((a2 % 2) * 4 + a1) * 4 + core * 2 + a2 // 2

    loads[0].wait()
    rt[R, :] = basis[R, :].astype(BF16)

    def core_parts(p):
        if p < 2:
            loads[1 + p].wait()
        for k in range(4):
            for j in range(4):
                block = part_block(p, STEPS[k], STEPS[j], 1 - c)
                s0s[p, k, j] = nn(rt[group[p], :], dens[p][:, lanes(block)]).astype(BF16)
            if p == 0 and k == 0:
                pl.semaphore_wait(barrier, len(peers))
            send(s0s.at[p, k], s0r.at[p, k], sx.at[0], s0y.at[p, k] if p < 2 else s0q.at[p - 2], other)

    def own_parts(p):
        for k in range(4):
            for j in range(4):
                block = part_block(p, STEPS[k], STEPS[j], c)
                acc[p, k, j] = nn(rt[group[p], :], dens[p][:, lanes(block)])

    def first_axis(p):
        if p > 1:
            landed(s0r.at[p], s0q.at[p - 2])
        for k in range(4):
            if p < 2:
                landed(s0r.at[p, k], s0y.at[p, k])
            for j in range(4):
                v = acc[p, k, j] + s0r[p, k, j].astype(F32)
                if k == 0:
                    rls[p, j] = v.astype(BF16)
                    send(rls.at[p, j], rlr.at[p, j], sx.at[1], rly.at[p, j] if p < 2 else rlq.at[p - 2],
                         along(first[p], 1 if j < 2 else 3))
                elif k == 1 and j >= 2:
                    ring(p, 0, j, v)
                elif k == 2 and j < 2:
                    ring(p, 1, j, v)
                else:
                    acc[p, k, j] = v

    def ring(p, way, j, v):
        s1s[p, way, j] = v.astype(BF16)
        send(s1s.at[p, way, j], s1r.at[p, way, j], sx.at[2],
             s1y.at[p, way, j] if p < 2 else s1q.at[p - 2], along(first[p], (1, 3)[way]))

    def relay(p):
        if p > 1:
            landed(rlr.at[p], rlq.at[p - 2])
        for j in (0, 2, 1, 3):
            way = 0 if j < 2 else 1
            if p < 2:
                landed(rlr.at[p, j], rly.at[p, j])
            ring(p, way, j, acc[p, 1 + way, j] + rlr[p, j].astype(F32))

    def second_axis(p):
        for j in (0, 2, 1, 3):
            v = acc[p, 3, j]
            for way in range(2):
                landed(s1r.at[p, way, j], s1y.at[p, way, j])
                v = v + s1r[p, way, j].astype(F32)
            if j == 3:
                acc[p, 3, j] = v
            else:
                s2s[p, j] = v.astype(BF16)
                send(s2s.at[p, j], s2r.at[p, j], sx.at[3], s2y.at[p], along(second[p], STEPS[j]))

    def gram_rows(p):
        landed(s1r.at[p], s1q.at[p - 2])
        for j in range(4):
            v = acc[p, 3, j]
            for way in range(2):
                v = v + s1r[p, way, j].astype(F32)
            qb[j, group[p], :] = v.astype(BF16)

    def third_axis(p):
        v = acc[p, 3, 3]
        landed(s2r.at[p], s2y.at[p])
        for j in range(3):
            v = v + s2r[p, j].astype(F32)
        acc[p, 3, 3] = v
        s3s[p] = v.astype(BF16)
        for k in range(3):
            send(s3s.at[p], s3r.at[p, k], sx.at[4], s3y.at[p], along(third[p], FAR[k]))

    def total(p):
        v = acc[p, 3, 3]
        landed(s3r.at[p], s3y.at[p])
        for k in range(3):
            v = v + s3r[p, k].astype(F32)
        return v

    BACK = (0,) + FAR
    BACKZ = (0, 1, 3, 2)
    row = ("y", "y")
    col = ("z", "z")

    def gat_block(p, m, kz, core):
        g1 = (at[row[p]] + 4 - BACK[m]) % 4
        g2 = (at[col[p]] + 4 - BACKZ[kz]) % 4
        if p == 0:
            return ((g1 % 2) * 4 + g2) * 4 + core * 2 + g1 // 2
        return core * 16 + g1 * 4 + g2

    def pass_on(p, m, kz):
        ref = gat.at[p, gat_block(p, m, kz, c)]
        send(ref, ref, sx.at[9 + p], a3y.at[p, min(kz, 1)], other)
        if m == 0 and kz == 0:
            for k in range(3):
                send(ref, ref, sx.at[9 + p], a1y.at[p, k], along(row[p], FAR[k]))
        if (kz == 0 and m % 2 == 1) or (kz == 2 and m % 2 == 0):
            send(ref, ref, sx.at[9 + p], a2y.at[p, 2, m], along(col[p], 2 if kz == 0 else 3))
        if kz == 0:
            for way in range(2):
                send(ref, ref, sx.at[9 + p], a2y.at[p, way, m], along(col[p], (1, 3)[way]))

    def use(p, core, pairs):
        term = None
        for m, kz in pairs:
            block = gat_block(p, m, kz, core)
            part = nt(gat[p, block], dens[p][:, lanes(block)])
            term = part if term is None else term + part
        return term

    ROW = [(m, 0) for m in range(4)]
    REST = [(m, kz) for kz in (1, 2) for m in range(4)] + [(m, 3) for m in range(4)]

    def gather_y(p):
        for m in (2, 3, 1):
            landed(gat.at[p, gat_block(p, m, 0, c)], a1y.at[p, m - 1])
            pass_on(p, m, 0)

    def gather_near(p):
        for m in (0, 2, 3, 1):
            for kz in (2, 1):
                landed(gat.at[p, gat_block(p, m, kz, c)], a2y.at[p, kz - 1, m])
                pass_on(p, m, kz)

    def gather_far(p, which):
        for m in which:
            landed(gat.at[p, gat_block(p, m, 3, c)], a2y.at[p, 2, m])
            pass_on(p, m, 3)

    def gather_core(p, rest):
        landed(gat.at[p, pl.ds(0, 12 if rest else 4)], a3y.at[p, rest])

    def share(buf, ssem, rsem, s, value):
        axis = "cxyz"[s]
        count = 2 if axis == "c" else 4
        here = c if axis == "c" else at[axis]
        buf[s, here] = value
        for k in range(count - 1):
            dev = other if axis == "c" else along(axis, FAR[k])
            send(buf.at[s, here], buf.at[s, here], ssem.at[s], rsem.at[s], dev)

    def shared(buf, rsem, s):
        count = 2 if s == 0 else 4
        landed(buf.at[s, pl.ds(0, count - 1)], rsem.at[s])
        value = buf[s, 0]
        for i in range(1, count):
            value = value + buf[s, i]
        return value

    scope = jax.named_scope
    with scope("core_d"):
        core_parts(0)
    with scope("own_d"):
        own_parts(0)
    with scope("first_d"):
        first_axis(0)
    with scope("core_e"):
        core_parts(1)
    with scope("own_e"):
        own_parts(1)
    with scope("first_e"):
        first_axis(1)
    with scope("q_x"):
        for i in (4, 5):
            loads[i].wait()
        rt[X, :] = basis[X, :].astype(BF16)
        rt[S, :] = basis[S, :].astype(BF16)
        core_parts(2)
    with scope("relay_d"):
        relay(0)
    with scope("relay_e"):
        own_parts(2)
        relay(1)
    with scope("first_x"):
        first_axis(2)
        core_parts(3)
    with scope("second_d"):
        second_axis(0)
    with scope("early"):
        for i in (6, 7, 9, 10, 11, 12, 13):
            loads[i].wait()
        share(early, ex, ey, 0, jnp.concatenate(
            [exact(images[X, :], basis[...], NT), exact(images[S, :], basis[...], NT)], axis=0))
        own_parts(3)
    with scope("second_e"):
        second_axis(1)
    with scope("third_d"):
        third_axis(0)
    with scope("first_r"):
        first_axis(3)
        relay(2)
        core_parts(4)
        own_parts(4)
    with scope("third_e"):
        third_axis(1)

    with scope("early1"):
        share(early, ex, ey, 1, shared(early, ey, 0))

    with scope("seen"):
        tot = total(0)
        seen[y_lo] = tot.astype(BF16)
        send(seen.at[y_lo], seen.at[y_lo], sx.at[5], s4y, along("y", 5 - 2 * y_lo))
    with scope("mm_near"):
        loads[3].wait()
        for q in range(4):
            bacc[q] = nt(seen[y_lo], screen[pl.ds(q * COLS, COLS), lanes(y_lo)])
    with scope("first_s"):
        relay(3)
        first_axis(4)
    with scope("weighted"):
        tot = total(1)
        loads[8].wait()
        mine = gat_block(1, 0, 0, c)
        gat[1, mine] = (coulomb[:, lanes(mine)] * tot).astype(BF16)
    with scope("mm_far"):
        landed(seen.at[1 - y_lo], s4y)
        kept = []
        for i in (1, 0, 3, 2):
            core = c if i > 1 else 1 - c
            half = y_hi if i in (0, 2) else 1 - y_hi
            q = core * 2 + half
            rows = pl.ds(pl.multiple_of(q * COLS, COLS), COLS)
            v = bacc[q] + nt(seen[1 - y_lo], screen[rows, lanes(1 - y_lo)])
            if i > 1:
                kept.append(v)
            else:
                c0s[i] = v.astype(BF16)
                send(c0s.at[i], c0r.at[i], sx.at[6], c0y.at[i], other)
        away, home = kept
        pass_on(1, 0, 0)
    with scope("rows_x"):
        gram_rows(2)

    with scope("c0"):
        for i in (1, 0):
            landed(c0r.at[i], c0y.at[i])
            if i == 1:
                c1s[...] = (away + c0r[1].astype(F32)).astype(BF16)
                send(c1s, c1r, sx.at[7], c1y, along("y", 2))
            else:
                home = home + c0r[0].astype(F32)
    with scope("relay_s"):
        relay(4)
        share(early, ex, ey, 2, shared(early, ey, 1))
    with scope("gather_y_e"):
        gather_y(1)
        exch = use(1, c, ROW)
        gram_rows(3)

    with scope("c1"):
        landed(c1r, c1y)
        home = home + c1r[...].astype(F32)
        c2s[...] = home.astype(BF16)
        for k in range(3):
            send(c2s, c2r.at[k], sx.at[8], c2y, along("x", FAR[k]))

    with scope("plain"):
        def pick(energy, index, count):
            hot = (lax.broadcasted_iota(jnp.int32, (count, ROWS), 0) == index[...]).astype(F32)
            return exact(energy[...], hot)

        gap = pick(con_e, con_i, con_e.shape[1]) - pick(val_e, val_i, val_e.shape[1])
        all_coef = ritz[...]
        column = lax.broadcasted_iota(jnp.int32, all_coef.shape, 1)
        lower = jnp.where(column >= NE, all_coef, 0.0)
        o_trial[...] = exact(all_coef, basis[...])
        o_search[...] = exact(lower, basis[...])
        store(0, o_trial, h_trial)
        store(1, o_search, h_search)
        gram_rows(4)
    with scope("gather_near_e"):
        gather_near(1)

    with scope("c2"):
        landed(c2r, c2y)
        for k in range(3):
            home = home + c2r[k].astype(F32)
        gat[0, gat_block(0, 0, 0, c)] = home.astype(BF16)
        pass_on(0, 0, 0)

    with scope("gather_far_e"):
        gather_far(1, (0, 2, 3, 1))
        exch = exch + use(1, c, REST)
    with scope("gather_y_d"):
        gather_y(0)
    with scope("gather_core_e"):
        gather_core(1, 0)
        gather_core(1, 1)
        exch = exch + use(1, 1 - c, ROW + REST)
        near = gap * basis[R, :] + 2.0 * exch
        late_near = exact(near, basis[...], NT)

    with scope("gram_d"):
        part = None
        for m, j in ((0, 3), (1, 0), (2, 2), (3, 1)):
            term = nt(gat[0, gat_block(0, m, 0, c)], qb[j])
            part = term if part is None else part + term
        share(late, lx, ly, 0, late_near - part)
        direct = use(0, c, ROW)
    with scope("early3"):
        share(early, ex, ey, 3, shared(early, ey, 2))
    with scope("core_row_d"):
        gather_core(0, 0)
        direct = direct + use(0, 1 - c, ROW)
    with scope("late1"):
        share(late, lx, ly, 1, shared(late, ly, 0))
    with scope("gather_near_d"):
        gather_near(0)
    with scope("gather_far_d"):
        gather_far(0, (0, 2))
    with scope("late2"):
        share(late, lx, ly, 2, shared(late, ly, 1))
    with scope("gather_far2_d"):
        gather_far(0, (3, 1))
    with scope("rest_d"):
        direct = direct + use(0, c, REST)
        gram = shared(early, ey, 3)
    with scope("gather_core_d"):
        gather_core(0, 1)
        direct = direct + use(0, 1 - c, REST)
    with scope("late3"):
        share(late, lx, ly, 3, shared(late, ly, 2))
    with scope("image"):
        images[R, :] = near - direct
        o_trial_img[...] = exact(all_coef, images[...])
        o_search_img[...] = exact(lower, images[...])
        store(2, o_trial_img, h_trial_img)
        store(3, o_search_img, h_search_img)
    with scope("late4"):
        mid = shared(late, ly, 3)
        gram = jnp.concatenate([gram[0:NE], mid, gram[NE:2 * NE]], axis=0)
        o_gram[...] = jnp.transpose(gram)
        store(4, o_gram, h_gram)

    with jax.named_scope("drain"):
        for i, ref in enumerate((
            s0s, rls, s1s, s2s, s3r, seen.at[0], c0s, c1s, c2r,
            gat.at[0, pl.ds(0, 31)], gat.at[1, pl.ds(0, 31)],
        )):
            left(ref, sx.at[i])
        for i in range(4):
            count = 1 if i == 0 else 3
            left(early.at[i, pl.ds(0, count)], ex.at[i])
            left(late.at[i, pl.ds(0, count)], lx.at[i])
        for copy in stores:
            copy.wait()


def put(*refs):
    n = len(refs) // 2
    sem = refs[-1]
    copies = [pltpu.make_async_copy(refs[i], refs[n + i], sem.at[i]) for i in range(n)]
    for copy in copies:
        copy.start()
    for copy in copies:
        copy.wait()


def solution(mesh):
    def body(trial, resid, search, trial_img, search_img, dens_e, dens_d, screen,
             coulomb, val_e, con_e, val_i, con_i, ritz):
        args = (trial.T, resid.T, search.T, trial_img.T, search_img.T, dens_e, dens_d, screen,
                coulomb.reshape(1, -1), val_e.reshape(1, -1), con_e.reshape(1, -1),
                val_i.reshape(1, -1), con_i.reshape(1, -1), ritz.T)
        dma = pltpu.SemaphoreType.DMA
        block = (NE, COLS)
        tall = pltpu.VMEM((3 * NE, ROWS), F32)
        flat = pltpu.VMEM((NE, ROWS), F32)
        scratch = [flat, flat, flat, flat, pltpu.VMEM((3 * NE, 3 * NE), F32), tall, tall] + [pltpu.VMEM(a.shape, a.dtype) for a in args[5:]] + [
            pltpu.VMEM((3 * NE, ROWS), BF16),
            pltpu.VMEM((5, 4, 4) + block, BF16),
            pltpu.VMEM((5, 4, 4) + block, BF16),
            pltpu.VMEM((5, 4, 4) + block, F32),
            pltpu.VMEM((5, 4) + block, BF16),
            pltpu.VMEM((5, 4) + block, BF16),
            pltpu.VMEM((5, 2, 4) + block, BF16),
            pltpu.VMEM((5, 2, 4) + block, BF16),
            pltpu.VMEM((2, 3) + block, BF16),
            pltpu.VMEM((2, 3) + block, BF16),
            pltpu.VMEM((2,) + block, BF16),
            pltpu.VMEM((2, 3) + block, BF16),
            pltpu.VMEM((4, 3 * NE, COLS), BF16),
            pltpu.VMEM((2,) + block, BF16),
            pltpu.VMEM((4,) + block, F32),
            pltpu.VMEM((2,) + block, BF16),
            pltpu.VMEM((2,) + block, BF16),
            pltpu.VMEM(block, BF16),
            pltpu.VMEM(block, BF16),
            pltpu.VMEM(block, BF16),
            pltpu.VMEM((3,) + block, BF16),
            pltpu.VMEM((2, 32) + block, BF16),
            pltpu.VMEM((4, 4, 2 * NE, 3 * NE), F32),
            pltpu.VMEM((4, 4, NE, 3 * NE), F32),
            dma((14,)), dma((5,)), dma((11,)), dma((4,)), dma((4,)),
            dma((2, 4)), dma((3,)), dma((2, 4)), dma((3,)), dma((2, 2, 4)), dma((3,)),
            dma((2,)), dma((2,)), dma, dma((2,)), dma, dma,
            dma((2, 3)), dma((2, 3, 4)), dma((2, 2)), dma((4,)), dma((4,)),
        ]
        vec = jax.ShapeDtypeStruct((NE, ROWS), F32)
        outs = (vec, vec, vec, vec, jax.ShapeDtypeStruct((3 * NE, 3 * NE), F32))
        parts = pl.pallas_call(
            kernel,
            out_shape=outs,
            in_specs=[pl.BlockSpec(memory_space=pl.ANY)] * len(args),
            out_specs=[pl.BlockSpec(memory_space=pl.ANY)] * 5,
            scratch_shapes=scratch,
            compiler_params=pltpu.CompilerParams(
                collective_id=0, has_side_effects=True, vmem_limit_bytes=67043328
            ),
            name="step",
        )(*args)
        parts = pl.pallas_call(
            put,
            out_shape=outs,
            in_specs=[pl.BlockSpec(memory_space=pltpu.VMEM)] * 5,
            out_specs=[pl.BlockSpec(memory_space=pl.ANY)] * 5,
            scratch_shapes=[dma((5,))],
            compiler_params=pltpu.CompilerParams(vmem_limit_bytes=67043328),
            name="put",
        )(*parts)
        return tuple(a.T for a in parts[:4]) + (parts[4],)

    both = P(("blk", "grp"), None)
    one = P(("blk", "grp"))
    return jax.shard_map(
        body,
        mesh=mesh,
        in_specs=(both,) * 7 + (P("grp", "blk"), P(None), P(None), P(None), one, one, P(None, None)),
        out_specs=(both,) * 4 + (P(None, None),),
        check_vma=False,
    )
```

```python
import jax
import jax.numpy as jnp
from jax import lax
from jax.experimental import pallas as pl
from jax.experimental.pallas import tpu as pltpu
from jax.sharding import PartitionSpec as P

NE = 24
ROWS = 48
NG = 20480
COLS = 640
MESH = pl.DeviceIdType.MESH
FAR = (2, 1, 3)
F32 = jnp.float32
BF16 = jnp.bfloat16
X, R, S = (pl.ds(i * NE, NE) for i in range(3))


NT = ((1,), (1,))


def exact(a, b, dims=((1,), (0,))):
    return lax.dot_general(
        a, b, (dims, ((), ())), precision=lax.Precision.HIGHEST, preferred_element_type=F32
    )


def nt(a, b):
    return lax.dot_general(a, b, (((1,), (1,)), ((), ())), preferred_element_type=F32)


def nn(a, b):
    return lax.dot_general(a, b, (((1,), (0,)), ((), ())), preferred_element_type=F32)


def kernel(
    trial_h, resid_h, search_h, trial_img_h, search_img_h, dens_e_h, dens_d_h, screen_h,
    coulomb_h, val_e_h, con_e_h, val_i_h, con_i_h, ritz_h,
    o_trial, o_trial_img, o_search, o_search_img, o_gram,
    basis, images, dens_e, dens_d, screen, coulomb, val_e, con_e, val_i, con_i, ritz,
    rt, s0s, s0r, acc, rls, rlr, s1s, s1r, s2s, s2r, s3s, s3r,
    qb, seen, bacc, c0s, c0r, c1s, c1r, c2s, c2r, gat, early, late,
    ld, sx, s0y, s0q, rly, rlq, s1y, s1q, s2y, s3y, s4y, c0y, c1y, c2y,
    a1y, a2y, a3y, ey, ly,
):
    blk = lax.axis_index("blk")
    grp = lax.axis_index("grp")
    c = blk % 2
    x = (blk // 2) % 4
    y_hi = blk // 8
    y_lo = grp // 4
    z = grp % 4
    y = y_hi * 2 + y_lo
    at = {"x": x, "y": y, "z": z, "c": c}

    def device(x=x, y=y, z=z, c=c):
        return ((y // 2) * 8 + x * 2 + c, (y % 2) * 4 + z)

    def along(axis, step):
        return device(**{axis: (at[axis] + step) % 4})

    other = device(c=1 - c)

    loads = []
    for i, (src, dst) in enumerate((
        (resid_h, basis.at[R]), (dens_d_h, dens_d), (dens_e_h, dens_e), (screen_h, screen),
        (coulomb_h, coulomb), (val_e_h, val_e), (con_e_h, con_e), (val_i_h, val_i),
        (con_i_h, con_i), (ritz_h, ritz),
    )):
        copy = pltpu.make_async_copy(src, dst, ld.at[i])
        copy.start()
        loads.append(copy)
    for i, (src, dst) in enumerate((
        (trial_h, basis.at[X]), (search_h, basis.at[S]),
        (trial_img_h, images.at[X]), (search_img_h, images.at[S]),
    )):
        pltpu.make_async_copy(src, dst, ld.at[10 + i // 2]).start()

    def pair_done(buf, sem):
        two = buf.at[pl.ds(0, 2 * NE)]
        pltpu.make_async_copy(two, two, sem).wait()

    barrier = pltpu.get_barrier_semaphore()
    peers = [other] + [along(a, d) for a in "xyz" for d in FAR]
    peers += [device(x=(x + d) % 4, c=1 - c) for d in FAR]
    for peer in peers:
        pl.semaphore_signal(barrier, inc=1, device_id=peer, device_id_type=MESH)

    def send(src, dst, ssem, rsem, dev):
        copy = pltpu.make_async_remote_copy(
            src_ref=src, dst_ref=dst, send_sem=ssem, recv_sem=rsem,
            device_id=dev, device_id_type=MESH,
        )
        copy.start()

    def landed(ref, rsem):
        pltpu.make_async_remote_copy(
            src_ref=ref, dst_ref=ref, send_sem=sx.at[0], recv_sem=rsem,
            device_id=other, device_id_type=MESH,
        ).wait_recv()

    def left(ref, ssem):
        pltpu.make_async_remote_copy(
            src_ref=ref, dst_ref=ref, send_sem=ssem, recv_sem=s4y,
            device_id=other, device_id_type=MESH,
        ).wait_send()

    STEPS = FAR + (0,)
    dens = (dens_d, dens_e, dens_d, dens_d, dens_d)
    group = (R, R, X, R, S)
    first = ("x", "z", "z", "z", "z")
    second = ("y",) * 5
    third = ("z", "x")

    def lanes(block):
        return pl.ds(pl.multiple_of(block * COLS, COLS), COLS)

    def part_block(p, step1, step2, core):
        a1 = (at[first[p]] + step1) % 4
        a2 = (at[second[p]] + step2) % 4
        if p == 0:
            return (a2 // 2) * 16 + a1 * 4 + core * 2 + a2 % 2
        if p == 1:
            return core * 16 + a2 * 4 + a1
        return ((a2 % 2) * 4 + a1) * 4 + core * 2 + a2 // 2

    loads[0].wait()
    rt[R, :] = basis[R, :].astype(BF16)

    def core_parts(p):
        if p < 2:
            loads[1 + p].wait()
        for k in range(4):
            for j in range(4):
                block = part_block(p, STEPS[k], STEPS[j], 1 - c)
                s0s[p, k, j] = nn(rt[group[p], :], dens[p][:, lanes(block)]).astype(BF16)
            if p == 0 and k == 0:
                pl.semaphore_wait(barrier, len(peers))
            send(s0s.at[p, k], s0r.at[p, k], sx.at[0], s0q.at[p - 2] if p > 1 else s0y.at[p, k], other)

    def own_parts(p):
        for k in range(4):
            for j in range(4):
                block = part_block(p, STEPS[k], STEPS[j], c)
                acc[p, k, j] = nn(rt[group[p], :], dens[p][:, lanes(block)])

    def first_axis(p):
        if p > 1:
            landed(s0r.at[p], s0q.at[p - 2])

        def chunk(k):
            if p < 2:
                landed(s0r.at[p, k], s0y.at[p, k])

        def both(k, j):
            return acc[p, k, j] + s0r[p, k, j].astype(F32)

        chunk(0)
        for j in (0, 2, 1, 3):
            rls[p, j] = both(0, j).astype(BF16)
            send(rls.at[p, j], rlr.at[p, j], sx.at[1], rlq.at[p - 2] if p > 1 else rly.at[p, j],
                 along(first[p], 1 if j < 2 else 3))
        chunk(1)
        chunk(2)
        for k, j in ((1, 2), (2, 0), (1, 3), (2, 1)):
            ring(p, k - 1, j, both(k, j))
        for k, j in ((1, 0), (2, 2), (1, 1), (2, 3)):
            acc[p, k, j] = both(k, j)
        chunk(3)
        for j in range(4):
            acc[p, 3, j] = both(3, j)

    def ring(p, way, j, v):
        s1s[p, way, j] = v.astype(BF16)
        send(s1s.at[p, way, j], s1r.at[p, way, j], sx.at[1],
             s1q.at[p - 2] if p > 1 else s1y.at[p, way, j], along(first[p], (1, 3)[way]))

    def relay(p):
        if p > 1:
            landed(rlr.at[p], rlq.at[p - 2])
        for j in (0, 2, 1, 3):
            way = 0 if j < 2 else 1
            if p < 2:
                landed(rlr.at[p, j], rly.at[p, j])
            ring(p, way, j, acc[p, 1 + way, j] + rlr[p, j].astype(F32))

    def second_axis(p):
        for j in (0, 2, 1, 3):
            v = acc[p, 3, j]
            for way in range(2):
                landed(s1r.at[p, way, j], s1y.at[p, way, j])
                v = v + s1r[p, way, j].astype(F32)
            if j == 3:
                acc[p, 3, j] = v
            else:
                s2s[p, j] = v.astype(BF16)
                send(s2s.at[p, j], s2r.at[p, j], sx.at[2], s2y.at[p], along(second[p], STEPS[j]))

    def gram_rows(p):
        landed(s1r.at[p], s1q.at[p - 2])
        for j in range(4):
            v = acc[p, 3, j]
            for way in range(2):
                v = v + s1r[p, way, j].astype(F32)
            qb[j, group[p], :] = v.astype(BF16)

    def third_axis(p):
        v = acc[p, 3, 3]
        landed(s2r.at[p], s2y.at[p])
        for j in range(3):
            v = v + s2r[p, j].astype(F32)
        acc[p, 3, 3] = v
        s3s[p] = v.astype(BF16)
        for k in (0, 2, 1):
            send(s3s.at[p], s3r.at[p, k], sx.at[2], s3y.at[p], along(third[p], FAR[k]))

    def total(p):
        v = acc[p, 3, 3]
        landed(s3r.at[p], s3y.at[p])
        for k in range(3):
            v = v + s3r[p, k].astype(F32)
        return v

    BACK = (0,) + FAR
    BACKZ = (0, 1, 3, 2)
    row = ("y", "y")
    col = ("z", "z")

    def gat_block(p, m, kz, core):
        g1 = (at[row[p]] + 4 - BACK[m]) % 4
        g2 = (at[col[p]] + 4 - BACKZ[kz]) % 4
        if p == 0:
            return ((g1 % 2) * 4 + g2) * 4 + core * 2 + g1 // 2
        return core * 16 + g1 * 4 + g2

    def pass_on(p, m, kz):
        ref = gat.at[p, gat_block(p, m, kz, c)]
        send(ref, ref, sx.at[3], a3y.at[p, min(kz, 1)], other)
        if m == 0 and kz == 0:
            for k in (0, 2, 1):
                send(ref, ref, sx.at[3], a1y.at[p, k], along(row[p], FAR[k]))
        if kz == 0:
            send(ref, ref, sx.at[3], a2y.at[p, 1, m], along(col[p], 3))
        if (kz == 0 and m % 2 == 1) or (kz == 2 and m % 2 == 0):
            send(ref, ref, sx.at[3], a2y.at[p, 2, m], along(col[p], 2 if kz == 0 else 3))
        if kz == 0:
            send(ref, ref, sx.at[3], a2y.at[p, 0, m], along(col[p], 1))

    def use(p, core, pairs):
        term = None
        for m, kz in pairs:
            block = gat_block(p, m, kz, core)
            part = nt(gat[p, block], dens[p][:, lanes(block)])
            term = part if term is None else term + part
        return term

    ROW = [(m, 0) for m in range(4)]
    REST = [(m, kz) for kz in (1, 2) for m in range(4)] + [(m, 3) for m in range(4)]

    def gather_y(p):
        for m in (2, 3, 1):
            landed(gat.at[p, gat_block(p, m, 0, c)], a1y.at[p, m - 1])
            pass_on(p, m, 0)

    def gather_near(p):
        for m in (0, 2, 3, 1):
            for kz in (2, 1):
                landed(gat.at[p, gat_block(p, m, kz, c)], a2y.at[p, kz - 1, m])
                pass_on(p, m, kz)

    def gather_far(p, which):
        for m in which:
            landed(gat.at[p, gat_block(p, m, 3, c)], a2y.at[p, 2, m])
            pass_on(p, m, 3)

    def gather_core(p, rest):
        landed(gat.at[p, pl.ds(0, 12 if rest else 4)], a3y.at[p, rest])

    HALF = (pl.ds(0, 384), pl.ds(384, 256))
    ROWS2 = ("y", "z")
    COLS2 = ("z", "y")

    def d_block(h, m, kz, core):
        g1 = (at[ROWS2[h]] + 4 - BACK[m]) % 4
        g2 = (at[COLS2[h]] + 4 - BACKZ[kz]) % 4
        yy, zz = (g1, g2) if h == 0 else (g2, g1)
        return ((yy % 2) * 4 + zz) * 4 + core * 2 + yy // 2

    def d_ref(h, m, kz):
        return gat.at[0, d_block(h, m, kz, c), :, HALF[h]]

    def d_row():
        for k in (0, 2, 1):
            for h in range(2):
                ref = d_ref(h, 0, 0)
                send(ref, ref, sx.at[4 + h], a1y.at[2 * h, k], along(ROWS2[h], FAR[k]))

    def d_pass(h, m, kz):
        ref = d_ref(h, m, kz)
        ssem = sx.at[4 + h]
        send(ref, ref, ssem, a3y.at[0, h], other)
        if kz == 0:
            send(ref, ref, ssem, a2y.at[2 * h, 1, m], along(COLS2[h], 3))
        if (kz == 0 and m < 2) or (kz == 2 and m > 1):
            send(ref, ref, ssem, a2y.at[2 * h, 2, m], along(COLS2[h], 2 if kz == 0 else 3))
        if kz == 0:
            send(ref, ref, ssem, a2y.at[2 * h, 0, m], along(COLS2[h], 1))

    def d_gather_row():
        for m in (2, 3, 1):
            for h in range(2):
                landed(d_ref(h, m, 0), a1y.at[2 * h, m - 1])
                d_pass(h, m, 0)

    def d_gather_near(which):
        for m in which:
            for h in range(2):
                for kz in (2, 1):
                    landed(d_ref(h, m, kz), a2y.at[2 * h, kz - 1, m])
                    d_pass(h, m, kz)

    def d_gather_far(which):
        for m in which:
            for h in range(2):
                landed(d_ref(h, m, 3), a2y.at[2 * h, 2, m])
                d_pass(h, m, 3)

    def spread(buf, sem, ssem, here, value, devices):
        buf[here] = value
        for dev in devices:
            send(buf.at[here], buf.at[here], ssem, sem, dev)

    def collected(buf, sem, count):
        landed(buf.at[pl.ds(0, count - 1)], sem)
        value = buf[0]
        for i in range(1, count):
            value = value + buf[i]
        return value

    def share_early(s, value):
        axis = "cxyz"[s]
        devices = [other] if s == 0 else [along(axis, d) for d in FAR]
        spread(early.at[s], ey.at[s], sx.at[6 if s == 0 else 7], at[axis], value, devices)

    def early_sum(s):
        return collected(early.at[s], ey.at[s], 4 if s else 2)

    LATE = (pl.ds(0, 8), pl.ds(8, 4), pl.ds(12, 4))

    def share_late(s, value):
        if s == 0:
            devices = [other] + [device(x=(x + d) % 4, c=k) for k in (1 - c, c) for d in (2, 3, 1)]
            here = x * 2 + c
        else:
            devices = [along("xyz"[s], d) for d in (2, 3, 1)]
            here = at["xyz"[s]]
        spread(late.at[LATE[s]], ly.at[s], sx.at[8 if s == 0 else 9], here, value, devices)

    def late_sum(s):
        return collected(late.at[LATE[s]], ly.at[s], 4 if s else 8)

    scope = jax.named_scope
    with scope("core_d"):
        core_parts(0)
    with scope("own_d"):
        own_parts(0)
    with scope("first_d"):
        first_axis(0)
    with scope("core_e"):
        core_parts(1)
    with scope("own_e"):
        own_parts(1)
    with scope("first_e"):
        first_axis(1)
    with scope("q_x"):
        pair_done(basis, ld.at[10])
        rt[X, :] = basis[X, :].astype(BF16)
        rt[S, :] = basis[S, :].astype(BF16)
        core_parts(2)
    with scope("relay_d"):
        relay(0)
    with scope("relay_e"):
        own_parts(2)
        relay(1)
    with scope("first_x"):
        first_axis(2)
        core_parts(3)
    with scope("second_d"):
        second_axis(0)
    with scope("early"):
        pair_done(images, ld.at[11])
        for i in range(5, 10):
            loads[i].wait()
        share_early(0, jnp.concatenate(
            [exact(images[X, :], basis[...], NT), exact(images[S, :], basis[...], NT)], axis=0))
        own_parts(3)
    with scope("second_e"):
        second_axis(1)
    with scope("third_d"):
        third_axis(0)
    with scope("first_r"):
        first_axis(3)
        relay(2)
        core_parts(4)
        own_parts(4)
    with scope("third_e"):
        third_axis(1)

    with scope("early1"):
        share_early(1, early_sum(0))

    with scope("seen"):
        tot = total(0)
        seen[y_lo] = tot.astype(BF16)
        send(seen.at[y_lo], seen.at[y_lo], sx.at[2], s4y, along("y", 5 - 2 * y_lo))
    with scope("mm_near"):
        loads[3].wait()
        for q in range(4):
            bacc[q] = nt(seen[y_lo], screen[pl.ds(q * COLS, COLS), lanes(y_lo)])
    with scope("first_s"):
        relay(3)
        first_axis(4)
    with scope("weighted"):
        tot = total(1)
        loads[4].wait()
        mine = gat_block(1, 0, 0, c)
        gat[1, mine] = (coulomb[:, lanes(mine)] * tot).astype(BF16)
    with scope("mm_far"):
        landed(seen.at[1 - y_lo], s4y)
        kept = []
        for i in (1, 0, 3, 2):
            core = c if i > 1 else 1 - c
            half = y_hi if i in (0, 2) else 1 - y_hi
            q = core * 2 + half
            rows = pl.ds(pl.multiple_of(q * COLS, COLS), COLS)
            v = bacc[q] + nt(seen[1 - y_lo], screen[rows, lanes(1 - y_lo)])
            if i > 1:
                kept.append(v)
            else:
                c0s[i] = v.astype(BF16)
                send(c0s.at[i], c0r.at[i], sx.at[2], c0y.at[i], other)
        away, home = kept
        pass_on(1, 0, 0)
    with scope("rows_x"):
        gram_rows(2)

    with scope("c0"):
        for i in (1, 0):
            landed(c0r.at[i], c0y.at[i])
            if i == 1:
                c1s[...] = (away + c0r[1].astype(F32)).astype(BF16)
                send(c1s, c1r, sx.at[2], c1y, along("y", 2))
            else:
                home = home + c0r[0].astype(F32)
    with scope("relay_s"):
        relay(4)
        share_early(2, early_sum(1))
    with scope("gather_y_e"):
        gather_y(1)
        exch = use(1, c, ROW)
        gram_rows(3)

    with scope("c1"):
        landed(c1r, c1y)
        home = home + c1r[...].astype(F32)
        c2s[...] = home.astype(BF16)
        for k in (0, 2, 1):
            send(c2s, c2r.at[k], sx.at[2], c2y, along("x", FAR[k]))

    with scope("plain"):
        def pick(energy, index, count):
            hot = (lax.broadcasted_iota(jnp.int32, (count, ROWS), 0) == index[...]).astype(F32)
            return exact(energy[...], hot)

        gap = pick(con_e, con_i, con_e.shape[1]) - pick(val_e, val_i, val_e.shape[1])
        all_coef = ritz[...]
        column = lax.broadcasted_iota(jnp.int32, all_coef.shape, 1)
        lower = jnp.where(column >= NE, all_coef, 0.0)
        o_trial[...] = exact(all_coef, basis[...])
        o_search[...] = exact(lower, basis[...])
        gram_rows(4)
    with scope("gather_near_e"):
        gather_near(1)

    with scope("c2"):
        landed(c2r, c2y)
        for k in range(3):
            home = home + c2r[k].astype(F32)
        gat[0, gat_block(0, 0, 0, c)] = home.astype(BF16)
        d_row()
        for h in range(2):
            d_pass(h, 0, 0)

    with scope("gather_far_e"):
        gather_far(1, (0, 2, 3, 1))
        exch = exch + use(1, c, REST)
    with scope("gather_y_d"):
        d_gather_row()
    with scope("gather_0_d"):
        d_gather_near((0,))
        d_gather_far((0,))
    with scope("gather_core_e"):
        gather_core(1, 0)
        gather_core(1, 1)
        exch = exch + use(1, 1 - c, ROW + REST)
        near = gap * basis[R, :] + 2.0 * exch
        late_near = exact(near, basis[...], NT)
    with scope("gram_d"):
        part = None
        for m, j in ((0, 3), (1, 0), (2, 2), (3, 1)):
            term = nt(gat[0, d_block(0, m, 0, c)], qb[j])
            part = term if part is None else part + term
        share_late(0, late_near - part)
    with scope("gather_near_d"):
        d_gather_near((2, 3, 1))
    with scope("late1"):
        share_late(1, late_sum(0))
    with scope("gather_far_d"):
        d_gather_far((1, 2, 3))
    with scope("rest_d"):
        direct = use(0, c, ROW + REST)
    with scope("early3"):
        share_early(3, early_sum(2))
    with scope("gather_core_d"):
        for h in range(2):
            landed(gat.at[0, pl.ds(0, 16), :, HALF[h]], a3y.at[0, h])
        direct = direct + use(0, 1 - c, ROW + REST)
    with scope("late2"):
        share_late(2, late_sum(1))
    with scope("image"):
        images[R, :] = near - direct
        o_trial_img[...] = exact(all_coef, images[...])
        o_search_img[...] = exact(lower, images[...])
    with scope("late4"):
        mid = late_sum(2)
        gram = early_sum(3)
        gram = jnp.concatenate([gram[0:NE], mid, gram[NE:2 * NE]], axis=0)
        o_gram[...] = jnp.transpose(gram)

    with jax.named_scope("drain"):
        for i, ref in enumerate((
            s0s, gat.at[:, pl.ds(0, 30)], gat.at[0, pl.ds(0, 19)], gat.at[1, pl.ds(0, 31)],
            gat.at[0, pl.ds(0, 31), :, HALF[0]], gat.at[0, pl.ds(0, 31), :, HALF[1]],
            early.at[0, 0], early.at[pl.ds(0, 3), pl.ds(0, 3)],
            late.at[pl.ds(0, 7)], late.at[pl.ds(0, 6)],
        )):
            left(ref, sx.at[i])


def put(*refs):
    n = len(refs) // 2
    sem = refs[-1]
    copies = [pltpu.make_async_copy(refs[i], refs[n + i], sem.at[i]) for i in range(n)]
    for copy in copies:
        copy.start()
    for copy in copies:
        copy.wait()


def solution(mesh):
    def body(trial, resid, search, trial_img, search_img, dens_e, dens_d, screen,
             coulomb, val_e, con_e, val_i, con_i, ritz):
        args = (trial.T, resid.T, search.T, trial_img.T, search_img.T, dens_e, dens_d, screen,
                coulomb.reshape(1, -1), val_e.reshape(1, -1), con_e.reshape(1, -1),
                val_i.reshape(1, -1), con_i.reshape(1, -1), ritz.T)
        args = tuple(pltpu.with_memory_space_constraint(a, pltpu.HBM) for a in args)
        dma = pltpu.SemaphoreType.DMA
        block = (NE, COLS)
        tall = pltpu.VMEM((3 * NE, ROWS), F32)
        scratch = [tall, tall] + [pltpu.VMEM(a.shape, a.dtype) for a in args[5:]] + [
            pltpu.VMEM((3 * NE, ROWS), BF16),
            pltpu.VMEM((5, 4, 4) + block, BF16),
            pltpu.VMEM((5, 4, 4) + block, BF16),
            pltpu.VMEM((5, 4, 4) + block, F32),
            pltpu.VMEM((5, 4) + block, BF16),
            pltpu.VMEM((5, 4) + block, BF16),
            pltpu.VMEM((5, 2, 4) + block, BF16),
            pltpu.VMEM((5, 2, 4) + block, BF16),
            pltpu.VMEM((2, 3) + block, BF16),
            pltpu.VMEM((2, 3) + block, BF16),
            pltpu.VMEM((2,) + block, BF16),
            pltpu.VMEM((2, 3) + block, BF16),
            pltpu.VMEM((4, 3 * NE, COLS), BF16),
            pltpu.VMEM((2,) + block, BF16),
            pltpu.VMEM((4,) + block, F32),
            pltpu.VMEM((2,) + block, BF16),
            pltpu.VMEM((2,) + block, BF16),
            pltpu.VMEM(block, BF16),
            pltpu.VMEM(block, BF16),
            pltpu.VMEM(block, BF16),
            pltpu.VMEM((3,) + block, BF16),
            pltpu.VMEM((2, 32) + block, BF16),
            pltpu.VMEM((4, 4, 2 * NE, 3 * NE), F32),
            pltpu.VMEM((16, NE, 3 * NE), F32),
            dma((12,)), dma((10,)),
            dma((2, 4)), dma((3,)), dma((2, 4)), dma((3,)), dma((2, 2, 4)), dma((3,)),
            dma((2,)), dma((2,)), dma, dma((2,)), dma, dma,
            dma((3, 3)), dma((3, 3, 4)), dma((2, 2)), dma((4,)), dma((3,)),
        ]
        vec = jax.ShapeDtypeStruct((NE, ROWS), F32)
        outs = (vec, vec, vec, vec, jax.ShapeDtypeStruct((3 * NE, 3 * NE), F32))
        parts = pl.pallas_call(
            kernel,
            out_shape=tuple(pltpu.VMEM(o.shape, F32) for o in outs),
            in_specs=[pl.BlockSpec(memory_space=pl.ANY)] * len(args),
            out_specs=[pl.BlockSpec(memory_space=pltpu.VMEM)] * 5,
            scratch_shapes=scratch,
            compiler_params=pltpu.CompilerParams(
                collective_id=0, has_side_effects=True, vmem_limit_bytes=56 * 1024 * 1024
            ),
            name="step",
        )(*args)
        parts = pl.pallas_call(
            put,
            out_shape=outs,
            in_specs=[pl.BlockSpec(memory_space=pltpu.VMEM)] * 5,
            out_specs=[pl.BlockSpec(memory_space=pl.ANY)] * 5,
            scratch_shapes=[dma((5,))],
            compiler_params=pltpu.CompilerParams(vmem_limit_bytes=1024 * 1024),
            name="put",
        )(*parts)
        return tuple(a.T for a in parts[:4]) + (parts[4],)

    both = P(("blk", "grp"), None)
    one = P(("blk", "grp"))
    return jax.shard_map(
        body,
        mesh=mesh,
        in_specs=(both,) * 7 + (P("grp", "blk"), P(None), P(None), P(None), one, one, P(None, None)),
        out_specs=(both,) * 4 + (P(None, None),),
        check_vma=False,
    )
```

```python
import jax
import jax.numpy as jnp
from jax import lax
from jax.experimental import pallas as pl
from jax.experimental.pallas import tpu as pltpu
from jax.sharding import PartitionSpec as P

NE = 24
ROWS = 48
NG = 20480
COLS = 640
MESH = pl.DeviceIdType.MESH
FAR = (2, 1, 3)
F32 = jnp.float32
BF16 = jnp.bfloat16
X, R, S = (pl.ds(i * NE, NE) for i in range(3))


NT = ((1,), (1,))


def exact(a, b, dims=((1,), (0,))):
    return lax.dot_general(
        a, b, (dims, ((), ())), precision=lax.Precision.HIGHEST, preferred_element_type=F32
    )


def nt(a, b):
    return lax.dot_general(a, b, (((1,), (1,)), ((), ())), preferred_element_type=F32)


def nn(a, b):
    return lax.dot_general(a, b, (((1,), (0,)), ((), ())), preferred_element_type=F32)


def kernel(
    trial_h, resid_h, search_h, trial_img_h, search_img_h, dens_e_h, dens_d_h, screen_h,
    coulomb_h, val_e_h, con_e_h, val_i_h, con_i_h, ritz_h,
    o_trial, o_trial_img, o_search, o_search_img, o_gram,
    basis, images, dens_e, dens_d, screen, coulomb, val_e, con_e, val_i, con_i, ritz,
    rt, s0s, s0r, acc, rls, rlr, s1s, s1r, s2s, s2r, s3s, s3r,
    qb, seen, bacc, c0s, c0r, c2s, c2r, gat, early, late,
    ld, sx, s0y, s0q, rly, rlq, s1y, s1q, s2y, s3y, s4y, c0y, c2y,
    a1y, a2y, a3y, ey, ly,
):
    blk = lax.axis_index("blk")
    grp = lax.axis_index("grp")
    c = blk % 2
    x = (blk // 2) % 4
    y_hi = blk // 8
    y_lo = grp // 4
    z = grp % 4
    y = y_hi * 2 + y_lo
    at = {"x": x, "y": y, "z": z, "c": c}

    def device(x=x, y=y, z=z, c=c):
        return ((y // 2) * 8 + x * 2 + c, (y % 2) * 4 + z)

    def along(axis, step):
        return device(**{axis: (at[axis] + step) % 4})

    other = device(c=1 - c)

    loads = []
    for i, (src, dst) in enumerate((
        (resid_h, basis.at[R]), (dens_d_h, dens_d), (dens_e_h, dens_e), (screen_h, screen),
        (coulomb_h, coulomb), (val_e_h, val_e), (con_e_h, con_e), (val_i_h, val_i),
        (con_i_h, con_i), (ritz_h, ritz),
    )):
        copy = pltpu.make_async_copy(src, dst, ld.at[i])
        copy.start()
        loads.append(copy)
    for i, (src, dst) in enumerate((
        (trial_h, basis.at[X]), (search_h, basis.at[S]),
        (trial_img_h, images.at[X]), (search_img_h, images.at[S]),
    )):
        pltpu.make_async_copy(src, dst, ld.at[10 + i // 2]).start()

    def pair_done(buf, sem):
        two = buf.at[pl.ds(0, 2 * NE)]
        pltpu.make_async_copy(two, two, sem).wait()

    barrier = pltpu.get_barrier_semaphore()
    peers = [other, device(y=(y + 2) % 4, c=1 - c)] + [along(a, d) for a in "xyz" for d in FAR]
    peers += [device(x=(x + d) % 4, c=1 - c) for d in FAR]
    for peer in peers:
        pl.semaphore_signal(barrier, inc=1, device_id=peer, device_id_type=MESH)

    def send(src, dst, ssem, rsem, dev):
        copy = pltpu.make_async_remote_copy(
            src_ref=src, dst_ref=dst, send_sem=ssem, recv_sem=rsem,
            device_id=dev, device_id_type=MESH,
        )
        copy.start()

    def landed(ref, rsem):
        pltpu.make_async_remote_copy(
            src_ref=ref, dst_ref=ref, send_sem=sx.at[0], recv_sem=rsem,
            device_id=other, device_id_type=MESH,
        ).wait_recv()

    def left(ref, ssem):
        pltpu.make_async_remote_copy(
            src_ref=ref, dst_ref=ref, send_sem=ssem, recv_sem=s4y,
            device_id=other, device_id_type=MESH,
        ).wait_send()

    STEPS = FAR + (0,)
    dens = (dens_d, dens_e, dens_d, dens_d, dens_d)
    group = (R, R, X, R, S)
    first = ("x", "z", "z", "z", "z")
    second = ("y",) * 5
    third = ("z", "x")

    def lanes(block):
        return pl.ds(pl.multiple_of(block * COLS, COLS), COLS)

    def part_block(p, step1, step2, core):
        a1 = (at[first[p]] + step1) % 4
        a2 = (at[second[p]] + step2) % 4
        if p == 0:
            return (a2 // 2) * 16 + a1 * 4 + core * 2 + a2 % 2
        if p == 1:
            return core * 16 + a2 * 4 + a1
        return ((a2 % 2) * 4 + a1) * 4 + core * 2 + a2 // 2

    loads[0].wait()
    rt[R, :] = basis[R, :].astype(BF16)

    def core_parts(p):
        if p < 2:
            loads[1 + p].wait()
        for k in range(4):
            for j in range(4):
                block = part_block(p, STEPS[k], STEPS[j], 1 - c)
                s0s[p, k, j] = nn(rt[group[p], :], dens[p][:, lanes(block)]).astype(BF16)
            if p == 0 and k == 0:
                pl.semaphore_wait(barrier, len(peers))
            send(s0s.at[p, k], s0r.at[p, k], sx.at[0], s0q.at[p - 2] if p > 1 else s0y.at[p, k], other)

    def own_parts(p):
        for k in range(4):
            for j in range(4):
                block = part_block(p, STEPS[k], STEPS[j], c)
                acc[p, k, j] = nn(rt[group[p], :], dens[p][:, lanes(block)])

    def first_axis(p):
        if p > 1:
            landed(s0r.at[p], s0q.at[p - 2])

        def chunk(k):
            if p < 2:
                landed(s0r.at[p, k], s0y.at[p, k])

        def both(k, j):
            return acc[p, k, j] + s0r[p, k, j].astype(F32)

        chunk(0)
        for j in (0, 2, 1, 3):
            rls[p, j] = both(0, j).astype(BF16)
            send(rls.at[p, j], rlr.at[p, j], sx.at[1], rlq.at[p - 2] if p > 1 else rly.at[p, j],
                 along(first[p], 1 if j < 2 else 3))
        chunk(1)
        chunk(2)
        for k, j in ((1, 2), (2, 0), (1, 3), (2, 1)):
            ring(p, k - 1, j, both(k, j))
        for k, j in ((1, 0), (2, 2), (1, 1), (2, 3)):
            acc[p, k, j] = both(k, j)
        chunk(3)
        for j in range(4):
            acc[p, 3, j] = both(3, j)

    def ring(p, way, j, v):
        s1s[p, way, j] = v.astype(BF16)
        send(s1s.at[p, way, j], s1r.at[p, way, j], sx.at[1],
             s1q.at[p - 2] if p > 1 else s1y.at[p, way, j], along(first[p], (1, 3)[way]))

    def relay(p):
        if p > 1:
            landed(rlr.at[p], rlq.at[p - 2])
        for j in (0, 2, 1, 3):
            way = 0 if j < 2 else 1
            if p < 2:
                landed(rlr.at[p, j], rly.at[p, j])
            ring(p, way, j, acc[p, 1 + way, j] + rlr[p, j].astype(F32))

    def second_axis(p):
        for j in (0, 2, 1, 3):
            v = acc[p, 3, j]
            for way in range(2):
                landed(s1r.at[p, way, j], s1y.at[p, way, j])
                v = v + s1r[p, way, j].astype(F32)
            if j == 3:
                acc[p, 3, j] = v
            else:
                s2s[p, j] = v.astype(BF16)
                send(s2s.at[p, j], s2r.at[p, j], sx.at[2], s2y.at[p], along(second[p], STEPS[j]))

    def gram_rows(p):
        landed(s1r.at[p], s1q.at[p - 2])
        for j in range(4):
            v = acc[p, 3, j]
            for way in range(2):
                v = v + s1r[p, way, j].astype(F32)
            qb[j, group[p], :] = v.astype(BF16)

    def third_axis(p):
        v = acc[p, 3, 3]
        landed(s2r.at[p], s2y.at[p])
        for j in range(3):
            v = v + s2r[p, j].astype(F32)
        acc[p, 3, 3] = v
        s3s[p] = v.astype(BF16)
        for k in (0, 2, 1):
            send(s3s.at[p], s3r.at[p, k], sx.at[2], s3y.at[p], along(third[p], FAR[k]))

    def total(p):
        v = acc[p, 3, 3]
        landed(s3r.at[p], s3y.at[p])
        for k in range(3):
            v = v + s3r[p, k].astype(F32)
        return v

    BACK = (0,) + FAR
    BACKZ = (0, 1, 3, 2)
    row = ("y", "y")
    col = ("z", "z")

    def gat_block(p, m, kz, core):
        g1 = (at[row[p]] + 4 - BACK[m]) % 4
        g2 = (at[col[p]] + 4 - BACKZ[kz]) % 4
        if p == 0:
            return ((g1 % 2) * 4 + g2) * 4 + core * 2 + g1 // 2
        return core * 16 + g1 * 4 + g2

    def pass_on(p, m, kz):
        ref = gat.at[p, gat_block(p, m, kz, c)]
        send(ref, ref, sx.at[3], a3y.at[p, min(kz, 1)], other)
        if m == 0 and kz == 0:
            for k in (0, 2, 1):
                send(ref, ref, sx.at[3], a1y.at[p, k], along(row[p], FAR[k]))
        if kz == 0:
            send(ref, ref, sx.at[3], a2y.at[p, 1, m], along(col[p], 3))
        if (kz == 0 and m % 2 == 1) or (kz == 2 and m % 2 == 0):
            send(ref, ref, sx.at[3], a2y.at[p, 2, m], along(col[p], 2 if kz == 0 else 3))
        if kz == 0:
            send(ref, ref, sx.at[3], a2y.at[p, 0, m], along(col[p], 1))

    def use(p, core, pairs):
        term = None
        for m, kz in pairs:
            block = gat_block(p, m, kz, core)
            part = nt(gat[p, block], dens[p][:, lanes(block)])
            term = part if term is None else term + part
        return term

    ROW = [(m, 0) for m in range(4)]
    REST = [(m, kz) for kz in (1, 2) for m in range(4)] + [(m, 3) for m in range(4)]

    def gather_y(p):
        for m in (2, 3, 1):
            landed(gat.at[p, gat_block(p, m, 0, c)], a1y.at[p, m - 1])
            pass_on(p, m, 0)

    def gather_near(p):
        for m in (0, 2, 3, 1):
            for kz in (2, 1):
                landed(gat.at[p, gat_block(p, m, kz, c)], a2y.at[p, kz - 1, m])
                pass_on(p, m, kz)

    def gather_far(p, which):
        for m in which:
            landed(gat.at[p, gat_block(p, m, 3, c)], a2y.at[p, 2, m])
            pass_on(p, m, 3)

    def gather_core(p, rest):
        landed(gat.at[p, pl.ds(0, 12 if rest else 4)], a3y.at[p, rest])

    HALF = (pl.ds(0, 384), pl.ds(384, 256))
    ROWS2 = ("y", "z")
    COLS2 = ("z", "y")

    def d_block(h, m, kz, core):
        g1 = (at[ROWS2[h]] + 4 - BACK[m]) % 4
        g2 = (at[COLS2[h]] + 4 - BACKZ[kz]) % 4
        yy, zz = (g1, g2) if h == 0 else (g2, g1)
        return ((yy % 2) * 4 + zz) * 4 + core * 2 + yy // 2

    def d_ref(h, m, kz):
        return gat.at[0, d_block(h, m, kz, c), :, HALF[h]]

    def d_row():
        for k in (0, 2, 1):
            for h in range(2):
                ref = d_ref(h, 0, 0)
                send(ref, ref, sx.at[4 + h], a1y.at[2 * h, k], along(ROWS2[h], FAR[k]))

    def d_pass(h, m, kz):
        ref = d_ref(h, m, kz)
        ssem = sx.at[4 + h]
        send(ref, ref, ssem, a3y.at[0, h], other)
        if kz == 0:
            send(ref, ref, ssem, a2y.at[2 * h, 1, m], along(COLS2[h], 3))
        if (kz == 0 and m < 2) or (kz == 2 and m > 1):
            send(ref, ref, ssem, a2y.at[2 * h, 2, m], along(COLS2[h], 2 if kz == 0 else 3))
        if kz == 0:
            send(ref, ref, ssem, a2y.at[2 * h, 0, m], along(COLS2[h], 1))

    def d_gather_row():
        for m in (2, 3, 1):
            for h in range(2):
                landed(d_ref(h, m, 0), a1y.at[2 * h, m - 1])
                d_pass(h, m, 0)

    def d_gather_near(which):
        for m in which:
            for h in range(2):
                for kz in (2, 1):
                    landed(d_ref(h, m, kz), a2y.at[2 * h, kz - 1, m])
                    d_pass(h, m, kz)

    def d_gather_far(which):
        for m in which:
            for h in range(2):
                landed(d_ref(h, m, 3), a2y.at[2 * h, 2, m])
                d_pass(h, m, 3)

    def spread(buf, sem, ssem, here, value, devices):
        buf[here] = value
        for dev in devices:
            send(buf.at[here], buf.at[here], ssem, sem, dev)

    def collected(buf, sem, count):
        landed(buf.at[pl.ds(0, count - 1)], sem)
        value = buf[0]
        for i in range(1, count):
            value = value + buf[i]
        return value

    def share_early(s, value):
        axis = "cxyz"[s]
        devices = [other] if s == 0 else [along(axis, d) for d in FAR]
        spread(early.at[s], ey.at[s], sx.at[6 if s == 0 else 7], at[axis], value, devices)

    def early_sum(s):
        return collected(early.at[s], ey.at[s], 4 if s else 2)

    LATE = (pl.ds(0, 8), pl.ds(8, 4), pl.ds(12, 4))

    def share_late(s, value):
        if s == 0:
            devices = [other] + [device(x=(x + d) % 4, c=k) for k in (1 - c, c) for d in (2, 3, 1)]
            here = x * 2 + c
        else:
            devices = [along("xyz"[s], d) for d in (2, 3, 1)]
            here = at["xyz"[s]]
        spread(late.at[LATE[s]], ly.at[s], sx.at[8 if s == 0 else 9], here, value, devices)

    def late_sum(s):
        return collected(late.at[LATE[s]], ly.at[s], 4 if s else 8)

    scope = jax.named_scope
    with scope("core_d"):
        core_parts(0)
    with scope("own_d"):
        own_parts(0)
    with scope("first_d"):
        first_axis(0)
    with scope("core_e"):
        core_parts(1)
    with scope("own_e"):
        own_parts(1)
    with scope("first_e"):
        first_axis(1)
    with scope("q_x"):
        pair_done(basis, ld.at[10])
        rt[X, :] = basis[X, :].astype(BF16)
        rt[S, :] = basis[S, :].astype(BF16)
        core_parts(2)
    with scope("relay_d"):
        relay(0)
    with scope("relay_e"):
        own_parts(2)
        relay(1)
    with scope("first_x"):
        first_axis(2)
        core_parts(3)
    with scope("second_d"):
        second_axis(0)
    with scope("early"):
        pair_done(images, ld.at[11])
        for i in range(5, 10):
            loads[i].wait()
        share_early(0, jnp.concatenate(
            [exact(images[X, :], basis[...], NT), exact(images[S, :], basis[...], NT)], axis=0))
        own_parts(3)
    with scope("second_e"):
        second_axis(1)
    with scope("third_d"):
        third_axis(0)
    with scope("first_r"):
        first_axis(3)
        relay(2)
        core_parts(4)
        own_parts(4)
    with scope("third_e"):
        third_axis(1)

    with scope("early1"):
        share_early(1, early_sum(0))

    with scope("seen"):
        tot = total(0)
        seen[y_lo] = tot.astype(BF16)
        send(seen.at[y_lo], seen.at[y_lo], sx.at[2], s4y, along("y", 5 - 2 * y_lo))
    with scope("mm_near"):
        loads[3].wait()
        for q in range(4):
            bacc[q] = nt(seen[y_lo], screen[pl.ds(q * COLS, COLS), lanes(y_lo)])
    with scope("first_s"):
        relay(3)
        first_axis(4)
    with scope("weighted"):
        tot = total(1)
        loads[4].wait()
        mine = gat_block(1, 0, 0, c)
        gat[1, mine] = (coulomb[:, lanes(mine)] * tot).astype(BF16)
        pass_on(1, 0, 0)
    with scope("mm_far"):
        landed(seen.at[1 - y_lo], s4y)
        across = (other, along("y", 2), device(y=(y + 2) % 4, c=1 - c))
        for i in (2, 1, 0, 3):
            core = c if i in (1, 3) else 1 - c
            half = y_hi if i in (0, 3) else 1 - y_hi
            q = core * 2 + half
            rows = pl.ds(pl.multiple_of(q * COLS, COLS), COLS)
            v = bacc[q] + nt(seen[1 - y_lo], screen[rows, lanes(1 - y_lo)])
            if i == 3:
                home = v
            else:
                c0s[i] = v.astype(BF16)
                send(c0s.at[i], c0r.at[i], sx.at[2], c0y, across[i])
    with scope("rows_x"):
        gram_rows(2)

    with scope("relay_s"):
        relay(4)
        share_early(2, early_sum(1))
    with scope("gather_y_e"):
        gather_y(1)
        exch = use(1, c, ROW)
        gram_rows(3)

    with scope("c1"):
        landed(c0r, c0y)
        for i in range(3):
            home = home + c0r[i].astype(F32)
        c2s[...] = home.astype(BF16)
        for k in (0, 2, 1):
            send(c2s, c2r.at[k], sx.at[2], c2y, along("x", FAR[k]))

    with scope("plain"):
        def pick(energy, index, count):
            hot = (lax.broadcasted_iota(jnp.int32, (count, ROWS), 0) == index[...]).astype(F32)
            return exact(energy[...], hot)

        gap = pick(con_e, con_i, con_e.shape[1]) - pick(val_e, val_i, val_e.shape[1])
        all_coef = ritz[...]
        column = lax.broadcasted_iota(jnp.int32, all_coef.shape, 1)
        lower = jnp.where(column >= NE, all_coef, 0.0)
        o_trial[...] = exact(all_coef, basis[...])
        o_search[...] = exact(lower, basis[...])
        gram_rows(4)
    with scope("gather_near_e"):
        gather_near(1)

    with scope("c2"):
        landed(c2r, c2y)
        for k in range(3):
            home = home + c2r[k].astype(F32)
        gat[0, gat_block(0, 0, 0, c)] = home.astype(BF16)
        d_row()
        for h in range(2):
            d_pass(h, 0, 0)

    with scope("gather_far_e"):
        gather_far(1, (0, 2, 3, 1))
        exch = exch + use(1, c, REST)
    with scope("gather_y_d"):
        d_gather_row()
    with scope("gather_0_d"):
        d_gather_near((0,))
        d_gather_far((0,))
    with scope("gather_core_e"):
        gather_core(1, 0)
        gather_core(1, 1)
        exch = exch + use(1, 1 - c, ROW + REST)
        near = gap * basis[R, :] + 2.0 * exch
        late_near = exact(near, basis[...], NT)
    with scope("gram_d"):
        part = None
        for m, j in ((0, 3), (1, 0), (2, 2), (3, 1)):
            term = nt(gat[0, d_block(0, m, 0, c)], qb[j])
            part = term if part is None else part + term
        share_late(0, late_near - part)
    with scope("gather_near_d"):
        d_gather_near((2, 3, 1))
    with scope("late1"):
        share_late(1, late_sum(0))
    with scope("gather_far_d"):
        d_gather_far((1, 2, 3))
    with scope("rest_d"):
        direct = use(0, c, ROW + REST)
    with scope("early3"):
        share_early(3, early_sum(2))
    with scope("gather_core_d"):
        for h in range(2):
            landed(gat.at[0, pl.ds(0, 16), :, HALF[h]], a3y.at[0, h])
        direct = direct + use(0, 1 - c, ROW + REST)
    with scope("late2"):
        share_late(2, late_sum(1))
    with scope("image"):
        images[R, :] = near - direct
        o_trial_img[...] = exact(all_coef, images[...])
        o_search_img[...] = exact(lower, images[...])
    with scope("late4"):
        mid = late_sum(2)
        gram = early_sum(3)
        gram = jnp.concatenate([gram[0:NE], mid, gram[NE:2 * NE]], axis=0)
        o_gram[...] = jnp.transpose(gram)

    with jax.named_scope("drain"):
        for i, ref in enumerate((
            s0s, gat.at[:, pl.ds(0, 30)], gat.at[0, pl.ds(0, 19)], gat.at[1, pl.ds(0, 31)],
            gat.at[0, pl.ds(0, 31), :, HALF[0]], gat.at[0, pl.ds(0, 31), :, HALF[1]],
            early.at[0, 0], early.at[pl.ds(0, 3), pl.ds(0, 3)],
            late.at[pl.ds(0, 7)], late.at[pl.ds(0, 6)],
        )):
            left(ref, sx.at[i])


def put(*refs):
    n = len(refs) // 2
    sem = refs[-1]
    copies = [pltpu.make_async_copy(refs[i], refs[n + i], sem.at[i]) for i in range(n)]
    for copy in copies:
        copy.start()
    for copy in copies:
        copy.wait()


def solution(mesh):
    def body(trial, resid, search, trial_img, search_img, dens_e, dens_d, screen,
             coulomb, val_e, con_e, val_i, con_i, ritz):
        args = (trial.T, resid.T, search.T, trial_img.T, search_img.T, dens_e, dens_d, screen,
                coulomb.reshape(1, -1), val_e.reshape(1, -1), con_e.reshape(1, -1),
                val_i.reshape(1, -1), con_i.reshape(1, -1), ritz.T)
        args = tuple(pltpu.with_memory_space_constraint(a, pltpu.HBM) for a in args)
        dma = pltpu.SemaphoreType.DMA
        block = (NE, COLS)
        tall = pltpu.VMEM((3 * NE, ROWS), F32)
        scratch = [tall, tall] + [pltpu.VMEM(a.shape, a.dtype) for a in args[5:]] + [
            pltpu.VMEM((3 * NE, ROWS), BF16),
            pltpu.VMEM((5, 4, 4) + block, BF16),
            pltpu.VMEM((5, 4, 4) + block, BF16),
            pltpu.VMEM((5, 4, 4) + block, F32),
            pltpu.VMEM((5, 4) + block, BF16),
            pltpu.VMEM((5, 4) + block, BF16),
            pltpu.VMEM((5, 2, 4) + block, BF16),
            pltpu.VMEM((5, 2, 4) + block, BF16),
            pltpu.VMEM((2, 3) + block, BF16),
            pltpu.VMEM((2, 3) + block, BF16),
            pltpu.VMEM((2,) + block, BF16),
            pltpu.VMEM((2, 3) + block, BF16),
            pltpu.VMEM((4, 3 * NE, COLS), BF16),
            pltpu.VMEM((2,) + block, BF16),
            pltpu.VMEM((4,) + block, F32),
            pltpu.VMEM((3,) + block, BF16),
            pltpu.VMEM((3,) + block, BF16),
            pltpu.VMEM(block, BF16),
            pltpu.VMEM((3,) + block, BF16),
            pltpu.VMEM((2, 32) + block, BF16),
            pltpu.VMEM((4, 4, 2 * NE, 3 * NE), F32),
            pltpu.VMEM((16, NE, 3 * NE), F32),
            dma((12,)), dma((10,)),
            dma((2, 4)), dma((3,)), dma((2, 4)), dma((3,)), dma((2, 2, 4)), dma((3,)),
            dma((2,)), dma((2,)), dma, dma, dma,
            dma((3, 3)), dma((3, 3, 4)), dma((2, 2)), dma((4,)), dma((3,)),
        ]
        vec = jax.ShapeDtypeStruct((NE, ROWS), F32)
        outs = (vec, vec, vec, vec, jax.ShapeDtypeStruct((3 * NE, 3 * NE), F32))
        parts = pl.pallas_call(
            kernel,
            out_shape=tuple(pltpu.VMEM(o.shape, F32) for o in outs),
            in_specs=[pl.BlockSpec(memory_space=pl.ANY)] * len(args),
            out_specs=[pl.BlockSpec(memory_space=pltpu.VMEM)] * 5,
            scratch_shapes=scratch,
            compiler_params=pltpu.CompilerParams(
                collective_id=0, has_side_effects=True, vmem_limit_bytes=56 * 1024 * 1024
            ),
            name="step",
        )(*args)
        parts = pl.pallas_call(
            put,
            out_shape=outs,
            in_specs=[pl.BlockSpec(memory_space=pltpu.VMEM)] * 5,
            out_specs=[pl.BlockSpec(memory_space=pl.ANY)] * 5,
            scratch_shapes=[dma((5,))],
            compiler_params=pltpu.CompilerParams(vmem_limit_bytes=1024 * 1024),
            name="put",
        )(*parts)
        return tuple(a.T for a in parts[:4]) + (parts[4],)

    both = P(("blk", "grp"), None)
    one = P(("blk", "grp"))
    return jax.shard_map(
        body,
        mesh=mesh,
        in_specs=(both,) * 7 + (P("grp", "blk"), P(None), P(None), P(None), one, one, P(None, None)),
        out_specs=(both,) * 4 + (P(None, None),),
        check_vma=False,
    )
```

```python
import jax
import jax.numpy as jnp
from jax import lax
from jax.experimental import pallas as pl
from jax.experimental.pallas import tpu as pltpu
from jax.sharding import PartitionSpec as P

NE = 24
ROWS = 48
NG = 20480
COLS = 640
MESH = pl.DeviceIdType.MESH
FAR = (2, 1, 3)
F32 = jnp.float32
BF16 = jnp.bfloat16
X, R, S = (pl.ds(i * NE, NE) for i in range(3))


NT = ((1,), (1,))


def exact(a, b, dims=((1,), (0,))):
    return lax.dot_general(
        a, b, (dims, ((), ())), precision=lax.Precision.HIGHEST, preferred_element_type=F32
    )


def nt(a, b):
    return lax.dot_general(a, b, (((1,), (1,)), ((), ())), preferred_element_type=F32)


def nn(a, b):
    return lax.dot_general(a, b, (((1,), (0,)), ((), ())), preferred_element_type=F32)


def kernel(
    trial_h, resid_h, search_h, trial_img_h, search_img_h, dens_e_h, dens_d_h, screen_h,
    coulomb_h, val_e_h, con_e_h, val_i_h, con_i_h, ritz_h,
    o_trial, o_trial_img, o_search, o_search_img, o_gram,
    basis, images, dens_e, dens_d, screen, coulomb, val_e, con_e, val_i, con_i, ritz,
    rt, s0s, s0r, acc, rls, rlr, s1s, s1r, s2s, s2r, s3s, s3r,
    qb, seen, bacc, c0s, c0r, c2s, c2r, gat, early, late,
    ld, sx, s0y, s0q, rly, rlq, s1y, s1q, s2y, s3y, s4y, c0y, c2y,
    a1y, a2y, d2y, a3y, ey, ly,
):
    blk = lax.axis_index("blk")
    grp = lax.axis_index("grp")
    c = blk % 2
    x = (blk // 2) % 4
    y_hi = blk // 8
    y_lo = grp // 4
    z = grp % 4
    y = y_hi * 2 + y_lo
    at = {"x": x, "y": y, "z": z, "c": c}

    def device(x=x, y=y, z=z, c=c):
        return ((y // 2) * 8 + x * 2 + c, (y % 2) * 4 + z)

    def along(axis, step):
        return device(**{axis: (at[axis] + step) % 4})

    other = device(c=1 - c)

    loads = []
    for i, (src, dst) in enumerate((
        (resid_h, basis.at[R]), (dens_d_h, dens_d), (dens_e_h, dens_e), (screen_h, screen),
        (coulomb_h, coulomb), (val_e_h, val_e), (con_e_h, con_e), (val_i_h, val_i),
        (con_i_h, con_i), (ritz_h, ritz),
    )):
        copy = pltpu.make_async_copy(src, dst, ld.at[i])
        copy.start()
        loads.append(copy)
    for i, (src, dst) in enumerate((
        (trial_h, basis.at[X]), (search_h, basis.at[S]),
        (trial_img_h, images.at[X]), (search_img_h, images.at[S]),
    )):
        pltpu.make_async_copy(src, dst, ld.at[10 + i // 2]).start()

    def pair_done(buf, sem):
        two = buf.at[pl.ds(0, 2 * NE)]
        pltpu.make_async_copy(two, two, sem).wait()

    barrier = pltpu.get_barrier_semaphore()
    peers = [other, device(y=(y + 2) % 4, c=1 - c)] + [along(a, d) for a in "xyz" for d in FAR]
    peers += [device(x=(x + d) % 4, c=1 - c) for d in FAR]
    for peer in peers:
        pl.semaphore_signal(barrier, inc=1, device_id=peer, device_id_type=MESH)

    def send(src, dst, ssem, rsem, dev):
        copy = pltpu.make_async_remote_copy(
            src_ref=src, dst_ref=dst, send_sem=ssem, recv_sem=rsem,
            device_id=dev, device_id_type=MESH,
        )
        copy.start()

    def landed(ref, rsem):
        pltpu.make_async_remote_copy(
            src_ref=ref, dst_ref=ref, send_sem=sx.at[0], recv_sem=rsem,
            device_id=other, device_id_type=MESH,
        ).wait_recv()

    def left(ref, ssem):
        pltpu.make_async_remote_copy(
            src_ref=ref, dst_ref=ref, send_sem=ssem, recv_sem=s4y,
            device_id=other, device_id_type=MESH,
        ).wait_send()

    STEPS = FAR + (0,)
    dens = (dens_d, dens_e, dens_d, dens_d, dens_d)
    group = (R, R, X, R, S)
    first = ("x", "z", "z", "z", "z")
    second = ("y",) * 5
    third = ("z", "x")

    def lanes(block):
        return pl.ds(pl.multiple_of(block * COLS, COLS), COLS)

    def part_block(p, step1, step2, core):
        a1 = (at[first[p]] + step1) % 4
        a2 = (at[second[p]] + step2) % 4
        if p == 0:
            return (a2 // 2) * 16 + a1 * 4 + core * 2 + a2 % 2
        if p == 1:
            return core * 16 + a2 * 4 + a1
        return ((a2 % 2) * 4 + a1) * 4 + core * 2 + a2 // 2

    loads[0].wait()
    rt[R, :] = basis[R, :].astype(BF16)

    def core_parts(p):
        if p < 2:
            loads[1 + p].wait()
        for k in range(4):
            for j in range(4):
                block = part_block(p, STEPS[k], STEPS[j], 1 - c)
                s0s[p, k, j] = nn(rt[group[p], :], dens[p][:, lanes(block)]).astype(BF16)
            if p == 0 and k == 0:
                pl.semaphore_wait(barrier, len(peers))
            send(s0s.at[p, k], s0r.at[p, k], sx.at[0], s0q.at[p - 2] if p > 1 else s0y.at[p, k], other)

    def own_parts(p):
        for k in range(4):
            for j in range(4):
                block = part_block(p, STEPS[k], STEPS[j], c)
                acc[p, k, j] = nn(rt[group[p], :], dens[p][:, lanes(block)])

    def first_axis(p):
        if p > 1:
            landed(s0r.at[p], s0q.at[p - 2])

        def chunk(k):
            if p < 2:
                landed(s0r.at[p, k], s0y.at[p, k])

        def both(k, j):
            return acc[p, k, j] + s0r[p, k, j].astype(F32)

        chunk(0)
        for j in (0, 2, 1, 3):
            rls[p, j] = both(0, j).astype(BF16)
            send(rls.at[p, j], rlr.at[p, j], sx.at[1], rlq.at[p - 2] if p > 1 else rly.at[p, j],
                 along(first[p], 1 if j < 2 else 3))
        chunk(1)
        chunk(2)
        for k, j in ((1, 2), (2, 0), (1, 3), (2, 1)):
            ring(p, k - 1, j, both(k, j))
        for k, j in ((1, 0), (2, 2), (1, 1), (2, 3)):
            acc[p, k, j] = both(k, j)
        chunk(3)
        for j in range(4):
            acc[p, 3, j] = both(3, j)

    def ring(p, way, j, v):
        s1s[p, way, j] = v.astype(BF16)
        send(s1s.at[p, way, j], s1r.at[p, way, j], sx.at[1],
             s1q.at[p - 2] if p > 1 else s1y.at[p, j], along(first[p], (1, 3)[way]))

    def relay(p):
        if p > 1:
            landed(rlr.at[p], rlq.at[p - 2])
        for j in (0, 2, 1, 3):
            way = 0 if j < 2 else 1
            if p < 2:
                landed(rlr.at[p, j], rly.at[p, j])
            ring(p, way, j, acc[p, 1 + way, j] + rlr[p, j].astype(F32))

    def second_axis(p):
        for j in (0, 2, 1, 3):
            v = acc[p, 3, j]
            landed(s1r.at[p, :, j], s1y.at[p, j])
            for way in range(2):
                v = v + s1r[p, way, j].astype(F32)
            if j == 3:
                acc[p, 3, j] = v
            else:
                s2s[p, j] = v.astype(BF16)
                send(s2s.at[p, j], s2r.at[p, j], sx.at[2], s2y.at[p], along(second[p], STEPS[j]))

    def gram_rows(p):
        landed(s1r.at[p], s1q.at[p - 2])
        for j in range(4):
            v = acc[p, 3, j]
            for way in range(2):
                v = v + s1r[p, way, j].astype(F32)
            qb[j, group[p], :] = v.astype(BF16)

    def third_axis(p):
        v = acc[p, 3, 3]
        landed(s2r.at[p], s2y.at[p])
        for j in range(3):
            v = v + s2r[p, j].astype(F32)
        acc[p, 3, 3] = v
        s3s[p] = v.astype(BF16)
        for k in (0, 2, 1):
            send(s3s.at[p], s3r.at[p, k], sx.at[2], s3y.at[p], along(third[p], FAR[k]))

    def total(p):
        v = acc[p, 3, 3]
        landed(s3r.at[p], s3y.at[p])
        for k in range(3):
            v = v + s3r[p, k].astype(F32)
        return v

    BACK = (0,) + FAR
    BACKZ = (0, 1, 3, 2)
    row = ("y", "y")
    col = ("z", "z")

    def gat_block(p, m, kz, core):
        g1 = (at[row[p]] + 4 - BACK[m]) % 4
        g2 = (at[col[p]] + 4 - BACKZ[kz]) % 4
        if p == 0:
            return ((g1 % 2) * 4 + g2) * 4 + core * 2 + g1 // 2
        return core * 16 + g1 * 4 + g2

    def pass_on(p, m, kz):
        ref = gat.at[p, gat_block(p, m, kz, c)]
        send(ref, ref, sx.at[3], a3y.at[p, min(kz, 1)], other)
        if m == 0 and kz == 0:
            for k in (0, 2, 1):
                send(ref, ref, sx.at[3], a1y.at[p, k], along(row[p], FAR[k]))
        if kz == 0:
            send(ref, ref, sx.at[3], a2y.at[1, m], along(col[p], 3))
        if (kz == 1 and m % 2 == 1) or (kz == 2 and m % 2 == 0):
            send(ref, ref, sx.at[3], a2y.at[2, m], along(col[p], 1 if kz == 1 else 3))
        if kz == 0:
            send(ref, ref, sx.at[3], a2y.at[0, m], along(col[p], 1))

    def use(p, core, pairs):
        term = None
        for m, kz in pairs:
            block = gat_block(p, m, kz, core)
            part = nt(gat[p, block], dens[p][:, lanes(block)])
            term = part if term is None else term + part
        return term

    ROW = [(m, 0) for m in range(4)]
    REST = [(m, kz) for kz in (1, 2) for m in range(4)] + [(m, 3) for m in range(4)]

    def gather_y(p):
        for m in (2, 3, 1):
            landed(gat.at[p, gat_block(p, m, 0, c)], a1y.at[p, m - 1])
            pass_on(p, m, 0)

    def gather_near(p):
        for m in (0, 2, 3, 1):
            for kz in (2, 1):
                landed(gat.at[p, gat_block(p, m, kz, c)], a2y.at[kz - 1, m])
                pass_on(p, m, kz)

    def gather_far(p, which):
        for m in which:
            landed(gat.at[p, gat_block(p, m, 3, c)], a2y.at[2, m])
            pass_on(p, m, 3)

    def gather_core(p, rest):
        landed(gat.at[p, pl.ds(0, 12 if rest else 4)], a3y.at[p, rest])

    HALF = (pl.ds(0, 384), pl.ds(384, 256))
    ROWS2 = ("y", "z")
    COLS2 = ("z", "y")

    def d_block(h, m, kz, core):
        g1 = (at[ROWS2[h]] + 4 - BACK[m]) % 4
        g2 = (at[COLS2[h]] + 4 - BACKZ[kz]) % 4
        yy, zz = (g1, g2) if h == 0 else (g2, g1)
        return ((yy % 2) * 4 + zz) * 4 + core * 2 + yy // 2

    def d_ref(h, m, kz):
        return gat.at[0, d_block(h, m, kz, c), :, HALF[h]]

    def d_row():
        for k in (0, 2, 1):
            for h in range(2):
                ref = d_ref(h, 0, 0)
                send(ref, ref, sx.at[4 + h], a1y.at[0, k], along(ROWS2[h], FAR[k]))

    def d_pass(h, m, kz):
        ref = d_ref(h, m, kz)
        ssem = sx.at[4 + h]
        send(ref, ref, ssem, a3y.at[0, h], other)
        if kz == 0:
            send(ref, ref, ssem, d2y.at[h, m], along(COLS2[h], 3))
        if kz == 0:
            send(ref, ref, ssem, d2y.at[2, m], along(COLS2[h], 2 if kz == 0 else 3))
        if kz == 0:
            send(ref, ref, ssem, d2y.at[h, m], along(COLS2[h], 1))

    def d_gather_row():
        for m in (2, 3, 1):
            landed(gat.at[0, 0], a1y.at[0, m - 1])
            for h in range(2):
                d_pass(h, m, 0)

    def d_gather_near(which):
        for m in which:
            for h in range(2):
                landed(gat.at[0, pl.ds(0, 2), :, HALF[h]], d2y.at[h, m])
                for kz in (2, 1):
                    d_pass(h, m, kz)

    def d_gather_far(which):
        for m in which:
            landed(gat.at[0, 0], d2y.at[2, m])
            for h in range(2):
                d_pass(h, m, 3)

    def spread(buf, sem, ssem, here, value, devices):
        buf[here] = value
        for dev in devices:
            send(buf.at[here], buf.at[here], ssem, sem, dev)

    def collected(buf, sem, count):
        landed(buf.at[pl.ds(0, count - 1)], sem)
        value = buf[0]
        for i in range(1, count):
            value = value + buf[i]
        return value

    def share_early(s, value):
        axis = "cxyz"[s]
        devices = [other] if s == 0 else [along(axis, d) for d in FAR]
        spread(early.at[s], ey.at[s], sx.at[6 if s == 0 else 7], at[axis], value, devices)

    def early_sum(s):
        return collected(early.at[s], ey.at[s], 4 if s else 2)

    LATE = (pl.ds(0, 8), pl.ds(8, 4), pl.ds(12, 4))

    def share_late(s, value):
        if s == 0:
            devices = [other] + [device(x=(x + d) % 4, c=k) for k in (1 - c, c) for d in (2, 3, 1)]
            here = x * 2 + c
        else:
            devices = [along("xyz"[s], d) for d in (2, 3, 1)]
            here = at["xyz"[s]]
        spread(late.at[LATE[s]], ly.at[s], sx.at[8 if s == 0 else 9], here, value, devices)

    def late_sum(s):
        return collected(late.at[LATE[s]], ly.at[s], 4 if s else 8)

    scope = jax.named_scope
    with scope("core_d"):
        core_parts(0)
    with scope("own_d"):
        own_parts(0)
    with scope("first_d"):
        first_axis(0)
    with scope("core_e"):
        core_parts(1)
    with scope("own_e"):
        own_parts(1)
    with scope("first_e"):
        first_axis(1)
    with scope("q_x"):
        pair_done(basis, ld.at[10])
        rt[X, :] = basis[X, :].astype(BF16)
        rt[S, :] = basis[S, :].astype(BF16)
        core_parts(2)
    with scope("relay_d"):
        relay(0)
    with scope("relay_e"):
        own_parts(2)
        relay(1)
    with scope("first_x"):
        first_axis(2)
        core_parts(3)
    with scope("second_d"):
        second_axis(0)
    with scope("early"):
        pair_done(images, ld.at[11])
        for i in range(5, 10):
            loads[i].wait()
        share_early(0, jnp.concatenate(
            [exact(images[X, :], basis[...], NT), exact(images[S, :], basis[...], NT)], axis=0))
        own_parts(3)
    with scope("second_e"):
        second_axis(1)
    with scope("third_d"):
        third_axis(0)
    with scope("first_r"):
        first_axis(3)
        relay(2)
        core_parts(4)
        own_parts(4)
    with scope("third_e"):
        third_axis(1)

    with scope("early1"):
        share_early(1, early_sum(0))

    with scope("seen"):
        tot = total(0)
        seen[y_lo] = tot.astype(BF16)
        send(seen.at[y_lo], seen.at[y_lo], sx.at[2], s4y, along("y", 5 - 2 * y_lo))
    with scope("mm_near"):
        loads[3].wait()
        for q in range(4):
            bacc[q] = nt(seen[y_lo], screen[pl.ds(q * COLS, COLS), lanes(y_lo)])
    with scope("first_s"):
        relay(3)
        first_axis(4)
    with scope("weighted"):
        tot = total(1)
        loads[4].wait()
        mine = gat_block(1, 0, 0, c)
        gat[1, mine] = (coulomb[:, lanes(mine)] * tot).astype(BF16)
        pass_on(1, 0, 0)
    with scope("mm_far"):
        landed(seen.at[1 - y_lo], s4y)
        across = (other, along("y", 2), device(y=(y + 2) % 4, c=1 - c))
        for i in (2, 1, 0, 3):
            core = c if i in (1, 3) else 1 - c
            half = y_hi if i in (0, 3) else 1 - y_hi
            q = core * 2 + half
            rows = pl.ds(pl.multiple_of(q * COLS, COLS), COLS)
            v = bacc[q] + nt(seen[1 - y_lo], screen[rows, lanes(1 - y_lo)])
            if i == 3:
                home = v
            else:
                c0s[i] = v.astype(BF16)
                send(c0s.at[i], c0r.at[i], sx.at[2], c0y, across[i])
    with scope("rows_x"):
        gram_rows(2)

    with scope("relay_s"):
        relay(4)
        share_early(2, early_sum(1))
    with scope("gather_y_e"):
        gather_y(1)
        exch = use(1, c, ROW)
        gram_rows(3)

    with scope("c1"):
        landed(c0r, c0y)
        for i in range(3):
            home = home + c0r[i].astype(F32)
        c2s[...] = home.astype(BF16)
        for k in (0, 2, 1):
            send(c2s, c2r.at[k], sx.at[2], c2y, along("x", FAR[k]))

    with scope("plain"):
        def pick(energy, index, count):
            hot = (lax.broadcasted_iota(jnp.int32, (count, ROWS), 0) == index[...]).astype(F32)
            return exact(energy[...], hot)

        gap = pick(con_e, con_i, con_e.shape[1]) - pick(val_e, val_i, val_e.shape[1])
        all_coef = ritz[...]
        column = lax.broadcasted_iota(jnp.int32, all_coef.shape, 1)
        lower = jnp.where(column >= NE, all_coef, 0.0)
        o_trial[...] = exact(all_coef, basis[...])
        o_search[...] = exact(lower, basis[...])
        gram_rows(4)
    with scope("gather_near_e"):
        gather_near(1)

    with scope("c2"):
        landed(c2r, c2y)
        for k in range(3):
            home = home + c2r[k].astype(F32)
        gat[0, gat_block(0, 0, 0, c)] = home.astype(BF16)
        d_row()
        for h in range(2):
            d_pass(h, 0, 0)

    with scope("gather_far_e"):
        gather_far(1, (0, 2, 3, 1))
        exch = exch + use(1, c, REST)
    with scope("gather_y_d"):
        d_gather_row()
    with scope("gather_0_d"):
        d_gather_near((0,))
        d_gather_far((0,))
    with scope("gather_core_e"):
        gather_core(1, 0)
        gather_core(1, 1)
        exch = exch + use(1, 1 - c, ROW + REST)
        near = gap * basis[R, :] + 2.0 * exch
        late_near = exact(near, basis[...], NT)
    with scope("gram_d"):
        part = None
        for m, j in ((0, 3), (1, 0), (2, 2), (3, 1)):
            term = nt(gat[0, d_block(0, m, 0, c)], qb[j])
            part = term if part is None else part + term
        share_late(0, late_near - part)
    with scope("gather_near_d"):
        d_gather_near((2, 3, 1))
    with scope("late1"):
        share_late(1, late_sum(0))
    with scope("gather_far_d"):
        d_gather_far((1, 2, 3))
    with scope("rest_d"):
        direct = use(0, c, ROW + REST)
    with scope("early3"):
        share_early(3, early_sum(2))
    with scope("gather_core_d"):
        for h in range(2):
            landed(gat.at[0, pl.ds(0, 16), :, HALF[h]], a3y.at[0, h])
        direct = direct + use(0, 1 - c, ROW + REST)
    with scope("late2"):
        share_late(2, late_sum(1))
    with scope("image"):
        images[R, :] = near - direct
        o_trial_img[...] = exact(all_coef, images[...])
        o_search_img[...] = exact(lower, images[...])
    with scope("late4"):
        mid = late_sum(2)
        gram = early_sum(3)
        gram = jnp.concatenate([gram[0:NE], mid, gram[NE:2 * NE]], axis=0)
        o_gram[...] = jnp.transpose(gram)

    with jax.named_scope("drain"):
        for i, ref in enumerate((
            s0s, gat.at[:, pl.ds(0, 30)], gat.at[0, pl.ds(0, 19)], gat.at[1, pl.ds(0, 31)],
            gat.at[0, pl.ds(0, 31), :, HALF[0]], gat.at[0, pl.ds(0, 31), :, HALF[1]],
            early.at[0, 0], early.at[pl.ds(0, 3), pl.ds(0, 3)],
            late.at[pl.ds(0, 7)], late.at[pl.ds(0, 6)],
        )):
            left(ref, sx.at[i])


def put(*refs):
    n = len(refs) // 2
    sem = refs[-1]
    copies = [pltpu.make_async_copy(refs[i], refs[n + i], sem.at[i]) for i in range(n)]
    for copy in copies:
        copy.start()
    for copy in copies:
        copy.wait()


def solution(mesh):
    def body(trial, resid, search, trial_img, search_img, dens_e, dens_d, screen,
             coulomb, val_e, con_e, val_i, con_i, ritz):
        args = (trial.T, resid.T, search.T, trial_img.T, search_img.T, dens_e, dens_d, screen,
                coulomb.reshape(1, -1), val_e.reshape(1, -1), con_e.reshape(1, -1),
                val_i.reshape(1, -1), con_i.reshape(1, -1), ritz.T)
        args = tuple(pltpu.with_memory_space_constraint(a, pltpu.HBM) for a in args)
        dma = pltpu.SemaphoreType.DMA
        block = (NE, COLS)
        tall = pltpu.VMEM((3 * NE, ROWS), F32)
        scratch = [tall, tall] + [pltpu.VMEM(a.shape, a.dtype) for a in args[5:]] + [
            pltpu.VMEM((3 * NE, ROWS), BF16),
            pltpu.VMEM((5, 4, 4) + block, BF16),
            pltpu.VMEM((5, 4, 4) + block, BF16),
            pltpu.VMEM((5, 4, 4) + block, F32),
            pltpu.VMEM((5, 4) + block, BF16),
            pltpu.VMEM((5, 4) + block, BF16),
            pltpu.VMEM((5, 2, 4) + block, BF16),
            pltpu.VMEM((5, 2, 4) + block, BF16),
            pltpu.VMEM((2, 3) + block, BF16),
            pltpu.VMEM((2, 3) + block, BF16),
            pltpu.VMEM((2,) + block, BF16),
            pltpu.VMEM((2, 3) + block, BF16),
            pltpu.VMEM((4, 3 * NE, COLS), BF16),
            pltpu.VMEM((2,) + block, BF16),
            pltpu.VMEM((4,) + block, F32),
            pltpu.VMEM((3,) + block, BF16),
            pltpu.VMEM((3,) + block, BF16),
            pltpu.VMEM(block, BF16),
            pltpu.VMEM((3,) + block, BF16),
            pltpu.VMEM((2, 32) + block, BF16),
            pltpu.VMEM((4, 4, 2 * NE, 3 * NE), F32),
            pltpu.VMEM((16, NE, 3 * NE), F32),
            dma((12,)), dma((10,)),
            dma((2, 4)), dma((3,)), dma((2, 4)), dma((3,)), dma((2, 4)), dma((3,)),
            dma((2,)), dma((2,)), dma, dma, dma,
            dma((2, 3)), dma((3, 4)), dma((3, 4)), dma((2, 2)), dma((4,)), dma((3,)),
        ]
        vec = jax.ShapeDtypeStruct((NE, ROWS), F32)
        outs = (vec, vec, vec, vec, jax.ShapeDtypeStruct((3 * NE, 3 * NE), F32))
        parts = pl.pallas_call(
            kernel,
            out_shape=tuple(pltpu.VMEM(o.shape, F32) for o in outs),
            in_specs=[pl.BlockSpec(memory_space=pl.ANY)] * len(args),
            out_specs=[pl.BlockSpec(memory_space=pltpu.VMEM)] * 5,
            scratch_shapes=scratch,
            compiler_params=pltpu.CompilerParams(
                collective_id=0, has_side_effects=True, vmem_limit_bytes=56 * 1024 * 1024
            ),
            name="step",
        )(*args)
        parts = pl.pallas_call(
            put,
            out_shape=outs,
            in_specs=[pl.BlockSpec(memory_space=pltpu.VMEM)] * 5,
            out_specs=[pl.BlockSpec(memory_space=pl.ANY)] * 5,
            scratch_shapes=[dma((5,))],
            compiler_params=pltpu.CompilerParams(vmem_limit_bytes=1024 * 1024),
            name="put",
        )(*parts)
        return tuple(a.T for a in parts[:4]) + (parts[4],)

    both = P(("blk", "grp"), None)
    one = P(("blk", "grp"))
    return jax.shard_map(
        body,
        mesh=mesh,
        in_specs=(both,) * 7 + (P("grp", "blk"), P(None), P(None), P(None), one, one, P(None, None)),
        out_specs=(both,) * 4 + (P(None, None),),
        check_vma=False,
    )
```

```python
import jax
import jax.numpy as jnp
from jax import lax
from jax.experimental import pallas as pl
from jax.experimental.pallas import tpu as pltpu
from jax.sharding import PartitionSpec as P

NE = 24
ROWS = 48
NG = 20480
COLS = 640
MESH = pl.DeviceIdType.MESH
FAR = (2, 1, 3)
F32 = jnp.float32
BF16 = jnp.bfloat16
X, R, S = (pl.ds(i * NE, NE) for i in range(3))


NT = ((1,), (1,))


def exact(a, b, dims=((1,), (0,))):
    return lax.dot_general(
        a, b, (dims, ((), ())), precision=lax.Precision.HIGHEST, preferred_element_type=F32
    )


def nt(a, b):
    return lax.dot_general(a, b, (((1,), (1,)), ((), ())), preferred_element_type=F32)


def nn(a, b):
    return lax.dot_general(a, b, (((1,), (0,)), ((), ())), preferred_element_type=F32)


def kernel(
    trial_h, resid_h, search_h, trial_img_h, search_img_h, dens_e_h, dens_d_h, screen_h,
    coulomb_h, val_e_h, con_e_h, val_i_h, con_i_h, ritz_h,
    o_trial, o_trial_img, o_search, o_search_img, o_gram,
    basis, images, dens_e, dens_d, screen, coulomb, val_e, con_e, val_i, con_i, ritz,
    rt, s0s, s0r, acc, rls, rlr, s1s, s1r, s2s, s2r, s3s, s3r,
    qb, seen, bacc, c0s, c0r, c2s, c2r, gat, early, late,
    ld, sx, s0y, s0q, rly, rlq, s1y, s1q, s2y, s3y, s4y, c0y, c2y,
    a1y, a2y, d2y, a3y, ey, ly,
):
    blk = lax.axis_index("blk")
    grp = lax.axis_index("grp")
    c = blk % 2
    x = (blk // 2) % 4
    y_hi = blk // 8
    y_lo = grp // 4
    z = grp % 4
    y = y_hi * 2 + y_lo
    at = {"x": x, "y": y, "z": z, "c": c}

    def device(x=x, y=y, z=z, c=c):
        return ((y // 2) * 8 + x * 2 + c, (y % 2) * 4 + z)

    def along(axis, step):
        return device(**{axis: (at[axis] + step) % 4})

    other = device(c=1 - c)

    loads = []
    for i, (src, dst) in enumerate((
        (resid_h, basis.at[R]), (dens_d_h, dens_d), (dens_e_h, dens_e), (screen_h, screen),
        (coulomb_h, coulomb), (val_e_h, val_e), (con_e_h, con_e), (val_i_h, val_i),
        (con_i_h, con_i), (ritz_h, ritz),
    )):
        copy = pltpu.make_async_copy(src, dst, ld.at[i])
        copy.start()
        loads.append(copy)
    for i, (src, dst) in enumerate((
        (trial_h, basis.at[X]), (search_h, basis.at[S]),
        (trial_img_h, images.at[X]), (search_img_h, images.at[S]),
    )):
        pltpu.make_async_copy(src, dst, ld.at[10 + i // 2]).start()

    def pair_done(buf, sem):
        two = buf.at[pl.ds(0, 2 * NE)]
        pltpu.make_async_copy(two, two, sem).wait()

    barrier = pltpu.get_barrier_semaphore()
    peers = [other, device(y=(y + 2) % 4, c=1 - c)] + [along(a, d) for a in "xyz" for d in FAR]
    peers += [device(x=(x + d) % 4, c=1 - c) for d in FAR]
    for peer in peers:
        pl.semaphore_signal(barrier, inc=1, device_id=peer, device_id_type=MESH)

    def send(src, dst, ssem, rsem, dev):
        copy = pltpu.make_async_remote_copy(
            src_ref=src, dst_ref=dst, send_sem=ssem, recv_sem=rsem,
            device_id=dev, device_id_type=MESH,
        )
        copy.start()

    def landed(ref, rsem):
        pltpu.make_async_remote_copy(
            src_ref=ref, dst_ref=ref, send_sem=sx.at[0], recv_sem=rsem,
            device_id=other, device_id_type=MESH,
        ).wait_recv()

    def left(ref, ssem):
        pltpu.make_async_remote_copy(
            src_ref=ref, dst_ref=ref, send_sem=ssem, recv_sem=s4y,
            device_id=other, device_id_type=MESH,
        ).wait_send()

    STEPS = FAR + (0,)
    dens = (dens_d, dens_e, dens_d, dens_d, dens_d)
    group = (R, R, X, R, S)
    first = ("x", "z", "z", "z", "z")
    second = ("y",) * 5
    third = ("z", "x")

    def lanes(block):
        return pl.ds(pl.multiple_of(block * COLS, COLS), COLS)

    def part_block(p, step1, step2, core):
        a1 = (at[first[p]] + step1) % 4
        a2 = (at[second[p]] + step2) % 4
        if p == 0:
            return (a2 // 2) * 16 + a1 * 4 + core * 2 + a2 % 2
        if p == 1:
            return core * 16 + a2 * 4 + a1
        return ((a2 % 2) * 4 + a1) * 4 + core * 2 + a2 // 2

    loads[0].wait()
    rt[R, :] = basis[R, :].astype(BF16)

    def core_parts(p):
        if p < 2:
            loads[1 + p].wait()
        for k in range(4):
            for j in range(4):
                block = part_block(p, STEPS[k], STEPS[j], 1 - c)
                s0s[p, k, j] = nn(rt[group[p], :], dens[p][:, lanes(block)]).astype(BF16)
            if p == 0 and k == 0:
                pl.semaphore_wait(barrier, len(peers))
            send(s0s.at[p, k], s0r.at[p, k], sx.at[0], s0q.at[p - 2] if p > 1 else s0y.at[p, k], other)

    def own_parts(p):
        for k in range(4):
            for j in range(4):
                block = part_block(p, STEPS[k], STEPS[j], c)
                acc[p, k, j] = nn(rt[group[p], :], dens[p][:, lanes(block)])

    def first_axis(p):
        if p > 1:
            landed(s0r.at[p], s0q.at[p - 2])

        def chunk(k):
            if p < 2:
                landed(s0r.at[p, k], s0y.at[p, k])

        def both(k, j):
            return acc[p, k, j] + s0r[p, k, j].astype(F32)

        chunk(0)
        for j in (0, 2, 1, 3):
            rls[p, j] = both(0, j).astype(BF16)
            send(rls.at[p, j], rlr.at[p, j], sx.at[1], rlq.at[p - 2] if p > 1 else rly.at[p, j],
                 along(first[p], 1 if j < 2 else 3))
        chunk(1)
        chunk(2)
        for k, j in ((1, 2), (2, 0), (1, 3), (2, 1)):
            ring(p, k - 1, j, both(k, j))
        for k, j in ((1, 0), (2, 2), (1, 1), (2, 3)):
            acc[p, k, j] = both(k, j)
        chunk(3)
        for j in range(4):
            acc[p, 3, j] = both(3, j)

    def ring(p, way, j, v):
        s1s[p, way, j] = v.astype(BF16)
        send(s1s.at[p, way, j], s1r.at[p, way, j], sx.at[1],
             s1q.at[p - 2] if p > 1 else s1y.at[p, j], along(first[p], (1, 3)[way]))

    def relay(p):
        if p > 1:
            landed(rlr.at[p], rlq.at[p - 2])
        for j in (0, 2, 1, 3):
            way = 0 if j < 2 else 1
            if p < 2:
                landed(rlr.at[p, j], rly.at[p, j])
            ring(p, way, j, acc[p, 1 + way, j] + rlr[p, j].astype(F32))

    def second_axis(p):
        for j in (0, 2, 1, 3):
            v = acc[p, 3, j]
            landed(s1r.at[p, :, j], s1y.at[p, j])
            for way in range(2):
                v = v + s1r[p, way, j].astype(F32)
            if j == 3:
                acc[p, 3, j] = v
            else:
                s2s[p, j] = v.astype(BF16)
                send(s2s.at[p, j], s2r.at[p, j], sx.at[2], s2y.at[p], along(second[p], STEPS[j]))

    def gram_rows(p):
        landed(s1r.at[p], s1q.at[p - 2])
        for j in range(4):
            v = acc[p, 3, j]
            for way in range(2):
                v = v + s1r[p, way, j].astype(F32)
            qb[j, group[p], :] = v.astype(BF16)

    def third_axis(p):
        v = acc[p, 3, 3]
        landed(s2r.at[p], s2y.at[p])
        for j in range(3):
            v = v + s2r[p, j].astype(F32)
        acc[p, 3, 3] = v
        s3s[p] = v.astype(BF16)
        for k in (0, 2, 1):
            send(s3s.at[p], s3r.at[p, k], sx.at[2], s3y.at[p], along(third[p], FAR[k]))

    def total(p):
        v = acc[p, 3, 3]
        landed(s3r.at[p], s3y.at[p])
        for k in range(3):
            v = v + s3r[p, k].astype(F32)
        return v

    BACK = (0,) + FAR
    BACKZ = (0, 1, 3, 2)
    row = ("y", "y")
    col = ("z", "z")

    def gat_block(p, m, kz, core):
        g1 = (at[row[p]] + 4 - BACK[m]) % 4
        g2 = (at[col[p]] + 4 - BACKZ[kz]) % 4
        if p == 0:
            return ((g1 % 2) * 4 + g2) * 4 + core * 2 + g1 // 2
        return core * 16 + g1 * 4 + g2

    def pass_on(p, m, kz):
        ref = gat.at[p, gat_block(p, m, kz, c)]
        send(ref, ref, sx.at[3], a3y.at[p, min(kz, 1)], other)
        if m == 0 and kz == 0:
            for k in (0, 2, 1):
                send(ref, ref, sx.at[3], a1y.at[p, k], along(row[p], FAR[k]))
        if kz == 0:
            send(ref, ref, sx.at[3], a2y.at[1, m], along(col[p], 3))
        if (kz == 1 and m % 2 == 1) or (kz == 2 and m % 2 == 0):
            send(ref, ref, sx.at[3], a2y.at[2, m], along(col[p], 1 if kz == 1 else 3))
        if kz == 0:
            send(ref, ref, sx.at[3], a2y.at[0, m], along(col[p], 1))

    def use(p, core, pairs):
        term = None
        for m, kz in pairs:
            block = gat_block(p, m, kz, core)
            part = nt(gat[p, block], dens[p][:, lanes(block)])
            term = part if term is None else term + part
        return term

    ROW = [(m, 0) for m in range(4)]
    REST = [(m, kz) for kz in (1, 2) for m in range(4)] + [(m, 3) for m in range(4)]

    def gather_y(p):
        for m in (2, 3, 1):
            landed(gat.at[p, gat_block(p, m, 0, c)], a1y.at[p, m - 1])
            pass_on(p, m, 0)

    def gather_near(p):
        for m in (0, 2, 3, 1):
            for kz in (2, 1):
                landed(gat.at[p, gat_block(p, m, kz, c)], a2y.at[kz - 1, m])
                pass_on(p, m, kz)

    def gather_far(p, which):
        for m in which:
            landed(gat.at[p, gat_block(p, m, 3, c)], a2y.at[2, m])
            pass_on(p, m, 3)

    def gather_core(p, rest):
        landed(gat.at[p, pl.ds(0, 12 if rest else 4)], a3y.at[p, rest])

    HALF = (pl.ds(0, 384), pl.ds(384, 256))
    ROWS2 = ("y", "z")
    COLS2 = ("z", "y")

    def d_block(h, m, kz, core):
        g1 = (at[ROWS2[h]] + 4 - BACK[m]) % 4
        g2 = (at[COLS2[h]] + 4 - BACKZ[kz]) % 4
        yy, zz = (g1, g2) if h == 0 else (g2, g1)
        return ((yy % 2) * 4 + zz) * 4 + core * 2 + yy // 2

    def d_ref(h, m, kz):
        return gat.at[0, d_block(h, m, kz, c), :, HALF[h]]

    def d_row():
        for k in (0, 2, 1):
            for h in range(2):
                ref = d_ref(h, 0, 0)
                send(ref, ref, sx.at[4 + h], a1y.at[0, k], along(ROWS2[h], FAR[k]))

    def d_pass(h, m, kz):
        ref = d_ref(h, m, kz)
        ssem = sx.at[4 + h]
        send(ref, ref, ssem, a3y.at[0, h], other)
        if kz == 0:
            send(ref, ref, ssem, d2y.at[h, m], along(COLS2[h], 3))
        if kz == 0:
            send(ref, ref, ssem, d2y.at[2, m], along(COLS2[h], 2 if kz == 0 else 3))
        if kz == 0:
            send(ref, ref, ssem, d2y.at[h, m], along(COLS2[h], 1))

    def d_gather_row():
        for m in (2, 3, 1):
            landed(gat.at[0, 0], a1y.at[0, m - 1])
            for h in range(2):
                d_pass(h, m, 0)

    def d_gather_near(which):
        for m in which:
            for h in range(2):
                landed(gat.at[0, pl.ds(0, 2), :, HALF[h]], d2y.at[h, m])
                for kz in (2, 1):
                    d_pass(h, m, kz)

    def d_gather_far(which):
        for m in which:
            landed(gat.at[0, 0], d2y.at[2, m])
            for h in range(2):
                d_pass(h, m, 3)

    def spread(buf, sem, ssem, here, value, devices):
        buf[here] = value
        for dev in devices:
            send(buf.at[here], buf.at[here], ssem, sem, dev)

    def collected(buf, sem, count):
        landed(buf.at[pl.ds(0, count - 1)], sem)
        value = buf[0]
        for i in range(1, count):
            value = value + buf[i]
        return value

    def share_early(s, value):
        axis = "cxyz"[s]
        devices = [other] if s == 0 else [along(axis, d) for d in FAR]
        spread(early.at[s], ey.at[s], sx.at[6 if s == 0 else 7], at[axis], value, devices)

    def early_sum(s):
        return collected(early.at[s], ey.at[s], 4 if s else 2)

    LATE = (pl.ds(0, 8), pl.ds(8, 4), pl.ds(12, 4))

    def share_late(s, value):
        if s == 0:
            devices = [other] + [device(x=(x + d) % 4, c=k) for k in (1 - c, c) for d in (2, 3, 1)]
            here = x * 2 + c
        else:
            devices = [along("xyz"[s], d) for d in (2, 3, 1)]
            here = at["xyz"[s]]
        spread(late.at[LATE[s]], ly.at[s], sx.at[8 if s == 0 else 9], here, value, devices)

    def late_sum(s):
        return collected(late.at[LATE[s]], ly.at[s], 4 if s else 8)

    scope = jax.named_scope
    with scope("core_d"):
        core_parts(0)
    with scope("own_d"):
        own_parts(0)
    with scope("first_d"):
        first_axis(0)
    with scope("core_e"):
        core_parts(1)
    with scope("own_e"):
        own_parts(1)
    with scope("first_e"):
        first_axis(1)
    with scope("q_x"):
        pair_done(basis, ld.at[10])
        rt[X, :] = basis[X, :].astype(BF16)
        rt[S, :] = basis[S, :].astype(BF16)
        core_parts(2)
    with scope("relay_d"):
        relay(0)
    with scope("relay_e"):
        own_parts(2)
        relay(1)
    with scope("first_x"):
        first_axis(2)
        core_parts(3)
    with scope("second_d"):
        second_axis(0)
    with scope("early"):
        pair_done(images, ld.at[11])
        for i in range(5, 10):
            loads[i].wait()
        share_early(0, jnp.concatenate(
            [exact(images[X, :], basis[...], NT), exact(images[S, :], basis[...], NT)], axis=0))
        own_parts(3)
    with scope("second_e"):
        second_axis(1)
    with scope("third_d"):
        third_axis(0)
    with scope("first_r"):
        first_axis(3)
        relay(2)
        core_parts(4)
        own_parts(4)
    with scope("third_e"):
        third_axis(1)

    with scope("early1"):
        share_early(1, early_sum(0))

    with scope("seen"):
        tot = total(0)
        seen[y_lo] = tot.astype(BF16)
        send(seen.at[y_lo], seen.at[y_lo], sx.at[2], s4y, along("y", 5 - 2 * y_lo))
    with scope("mm_near"):
        loads[3].wait()
        for q in range(4):
            bacc[q] = nt(seen[y_lo], screen[pl.ds(q * COLS, COLS), lanes(y_lo)])
    with scope("first_s"):
        relay(3)
        first_axis(4)
    with scope("weighted"):
        tot = total(1)
        loads[4].wait()
        mine = gat_block(1, 0, 0, c)
        gat[1, mine] = (coulomb[:, lanes(mine)] * tot).astype(BF16)
        pass_on(1, 0, 0)
    with scope("mm_far"):
        landed(seen.at[1 - y_lo], s4y)
        across = (other, along("y", 2), device(y=(y + 2) % 4, c=1 - c))
        for i in (2, 1, 0, 3):
            core = c if i in (1, 3) else 1 - c
            half = y_hi if i in (0, 3) else 1 - y_hi
            q = core * 2 + half
            rows = pl.ds(pl.multiple_of(q * COLS, COLS), COLS)
            v = bacc[q] + nt(seen[1 - y_lo], screen[rows, lanes(1 - y_lo)])
            if i == 3:
                home = v
            else:
                c0s[i] = v.astype(BF16)
                send(c0s.at[i], c0r.at[i], sx.at[2], c0y, across[i])
    with scope("rows_x"):
        gram_rows(2)

    with scope("relay_s"):
        relay(4)
        share_early(2, early_sum(1))
    with scope("gather_y_e"):
        gather_y(1)
        exch = use(1, c, ROW)
        gram_rows(3)

    with scope("c1"):
        landed(c0r, c0y)
        for i in range(3):
            home = home + c0r[i].astype(F32)
        c2s[...] = home.astype(BF16)
        for k in (0, 2, 1):
            send(c2s, c2r.at[k], sx.at[2], c2y, along("x", FAR[k]))

    with scope("plain"):
        def pick(energy, index, count):
            hot = (lax.broadcasted_iota(jnp.int32, (count, ROWS), 0) == index[...]).astype(F32)
            return exact(energy[...], hot)

        gap = pick(con_e, con_i, con_e.shape[1]) - pick(val_e, val_i, val_e.shape[1])
        all_coef = ritz[...]
        column = lax.broadcasted_iota(jnp.int32, all_coef.shape, 1)
        lower = jnp.where(column >= NE, all_coef, 0.0)
        o_trial[...] = exact(all_coef, basis[...])
        o_search[...] = exact(lower, basis[...])
        gram_rows(4)
    with scope("gather_near_e"):
        gather_near(1)

    with scope("c2"):
        landed(c2r, c2y)
        for k in range(3):
            home = home + c2r[k].astype(F32)
        gat[0, gat_block(0, 0, 0, c)] = home.astype(BF16)
        d_row()
        for h in range(2):
            d_pass(h, 0, 0)

    with scope("gather_far_e"):
        gather_far(1, (0, 2, 3, 1))
        exch = exch + use(1, c, REST)
        gather_core(1, 0)
        exch = exch + use(1, 1 - c, ROW)
    with scope("gather_y_d"):
        d_gather_row()
    with scope("gather_0_d"):
        d_gather_near((0,))
        d_gather_far((0,))
    with scope("gather_core_e"):
        gather_core(1, 1)
        exch = exch + use(1, 1 - c, REST)
        near = gap * basis[R, :] + 2.0 * exch
        late_near = exact(near, basis[...], NT)
    with scope("gram_d"):
        part = None
        for m, j in ((0, 3), (1, 0), (2, 2), (3, 1)):
            term = nt(gat[0, d_block(0, m, 0, c)], qb[j])
            part = term if part is None else part + term
        share_late(0, late_near - part)
    with scope("gather_near_d"):
        d_gather_near((2, 3, 1))
    with scope("late1"):
        share_late(1, late_sum(0))
    with scope("gather_far_d"):
        d_gather_far((1, 2, 3))
    with scope("rest_d"):
        direct = use(0, c, ROW + REST)
    with scope("early3"):
        share_early(3, early_sum(2))
    with scope("gather_core_d"):
        for h in range(2):
            landed(gat.at[0, pl.ds(0, 16), :, HALF[h]], a3y.at[0, h])
        direct = direct + use(0, 1 - c, ROW + REST)
    with scope("late2"):
        share_late(2, late_sum(1))
    with scope("image"):
        images[R, :] = near - direct
        o_trial_img[...] = exact(all_coef, images[...])
        o_search_img[...] = exact(lower, images[...])
    with scope("late4"):
        mid = late_sum(2)
        gram = early_sum(3)
        gram = jnp.concatenate([gram[0:NE], mid, gram[NE:2 * NE]], axis=0)
        o_gram[...] = jnp.transpose(gram)

    with jax.named_scope("drain"):
        for i, ref in enumerate((
            s0s, gat.at[:, pl.ds(0, 30)], gat.at[0, pl.ds(0, 19)], gat.at[1, pl.ds(0, 31)],
            gat.at[0, pl.ds(0, 31), :, HALF[0]], gat.at[0, pl.ds(0, 31), :, HALF[1]],
            early.at[0, 0], early.at[pl.ds(0, 3), pl.ds(0, 3)],
            late.at[pl.ds(0, 7)], late.at[pl.ds(0, 6)],
        )):
            left(ref, sx.at[i])


def put(*refs):
    n = len(refs) // 2
    sem = refs[-1]
    copies = [pltpu.make_async_copy(refs[i], refs[n + i], sem.at[i]) for i in range(n)]
    for copy in copies:
        copy.start()
    for copy in copies:
        copy.wait()


def solution(mesh):
    def body(trial, resid, search, trial_img, search_img, dens_e, dens_d, screen,
             coulomb, val_e, con_e, val_i, con_i, ritz):
        args = (trial.T, resid.T, search.T, trial_img.T, search_img.T, dens_e, dens_d, screen,
                coulomb.reshape(1, -1), val_e.reshape(1, -1), con_e.reshape(1, -1),
                val_i.reshape(1, -1), con_i.reshape(1, -1), ritz.T)
        args = tuple(pltpu.with_memory_space_constraint(a, pltpu.HBM) for a in args)
        dma = pltpu.SemaphoreType.DMA
        block = (NE, COLS)
        tall = pltpu.VMEM((3 * NE, ROWS), F32)
        scratch = [tall, tall] + [pltpu.VMEM(a.shape, a.dtype) for a in args[5:]] + [
            pltpu.VMEM((3 * NE, ROWS), BF16),
            pltpu.VMEM((5, 4, 4) + block, BF16),
            pltpu.VMEM((5, 4, 4) + block, BF16),
            pltpu.VMEM((5, 4, 4) + block, F32),
            pltpu.VMEM((5, 4) + block, BF16),
            pltpu.VMEM((5, 4) + block, BF16),
            pltpu.VMEM((5, 2, 4) + block, BF16),
            pltpu.VMEM((5, 2, 4) + block, BF16),
            pltpu.VMEM((2, 3) + block, BF16),
            pltpu.VMEM((2, 3) + block, BF16),
            pltpu.VMEM((2,) + block, BF16),
            pltpu.VMEM((2, 3) + block, BF16),
            pltpu.VMEM((4, 3 * NE, COLS), BF16),
            pltpu.VMEM((2,) + block, BF16),
            pltpu.VMEM((4,) + block, F32),
            pltpu.VMEM((3,) + block, BF16),
            pltpu.VMEM((3,) + block, BF16),
            pltpu.VMEM(block, BF16),
            pltpu.VMEM((3,) + block, BF16),
            pltpu.VMEM((2, 32) + block, BF16),
            pltpu.VMEM((4, 4, 2 * NE, 3 * NE), F32),
            pltpu.VMEM((16, NE, 3 * NE), F32),
            dma((12,)), dma((10,)),
            dma((2, 4)), dma((3,)), dma((2, 4)), dma((3,)), dma((2, 4)), dma((3,)),
            dma((2,)), dma((2,)), dma, dma, dma,
            dma((2, 3)), dma((3, 4)), dma((3, 4)), dma((2, 2)), dma((4,)), dma((3,)),
        ]
        vec = jax.ShapeDtypeStruct((NE, ROWS), F32)
        outs = (vec, vec, vec, vec, jax.ShapeDtypeStruct((3 * NE, 3 * NE), F32))
        parts = pl.pallas_call(
            kernel,
            out_shape=tuple(pltpu.VMEM(o.shape, F32) for o in outs),
            in_specs=[pl.BlockSpec(memory_space=pl.ANY)] * len(args),
            out_specs=[pl.BlockSpec(memory_space=pltpu.VMEM)] * 5,
            scratch_shapes=scratch,
            compiler_params=pltpu.CompilerParams(
                collective_id=0, has_side_effects=True, vmem_limit_bytes=56 * 1024 * 1024
            ),
            name="step",
        )(*args)
        parts = pl.pallas_call(
            put,
            out_shape=outs,
            in_specs=[pl.BlockSpec(memory_space=pltpu.VMEM)] * 5,
            out_specs=[pl.BlockSpec(memory_space=pl.ANY)] * 5,
            scratch_shapes=[dma((5,))],
            compiler_params=pltpu.CompilerParams(vmem_limit_bytes=1024 * 1024),
            name="put",
        )(*parts)
        return tuple(a.T for a in parts[:4]) + (parts[4],)

    both = P(("blk", "grp"), None)
    one = P(("blk", "grp"))
    return jax.shard_map(
        body,
        mesh=mesh,
        in_specs=(both,) * 7 + (P("grp", "blk"), P(None), P(None), P(None), one, one, P(None, None)),
        out_specs=(both,) * 4 + (P(None, None),),
        check_vma=False,
    )
```
